32 devices in a mesh: seq: 16 (over z, y, core), mp: 2 (over x).
Axes of the slice: x: 2, y: 2, z: 4, core: 2. Of those that a mesh axis runs over, the one named last changes fastest.
Arguments:
- query: bfloat16 [4096, 3072], P('seq', 'mp'), may hold values from -4.5 to 4.5
- key: bfloat16 [4096, 3072], P('seq', 'mp'), may hold values from -4.5 to 4.5
- value: bfloat16 [4096, 3072], P('seq', 'mp'), may hold values from -6 to 6
- clip_lengths: int32 [4, 4], replicated, may hold values from 0 to 1024, as said below
Outputs:
- attended: bfloat16 [4096, 3072], P(('seq', 'mp'))
The draws below stay inside these ranges and needn't reach their ends.
Inputs may be any that keep to these rules, and one draw needn't show every extreme that they name: `clip_lengths`: each row sums to 1024; a clip slot may be empty; in some bucket one clip fills all 1024 tokens.
All inputs are finite; a program needn't handle non-finite values.
Results may differ from the reference program's by a relative error of at most 0.01.
Values may be sent and summed in bfloat16 or wider, within the bound.
A program may use at most 64 MiB of HBM per device.

```python
import jax
import jax.numpy as jnp
from jax import lax

HD = 128
PER = 4
D = 3072
MOST = 1024
BUCKETS = 4
TOKENS = 4096


def draw_query(key, part):
    base = jax.random.normal(jax.random.fold_in(key, 1), (TOKENS, D), jnp.float32)
    return jnp.clip(base, -4.5, 4.5).astype(jnp.bfloat16)


def draw_key(key, part):
    base = jax.random.normal(jax.random.fold_in(key, 2), (TOKENS, D), jnp.float32)
    return jnp.clip(base, -4.5, 4.5).astype(jnp.bfloat16)


def draw_clip_lengths(key, part):
    cuts = jax.random.randint(jax.random.fold_in(key, 21), (BUCKETS, PER - 1), 0, MOST + 1).astype(jnp.int32)
    cuts = jnp.sort(cuts, axis=1)
    zeros = jnp.zeros((BUCKETS, 1), jnp.int32)
    filled = jnp.full((BUCKETS, 1), MOST, jnp.int32)
    lengths = jnp.diff(jnp.concatenate([zeros, cuts, filled], axis=1), axis=1)
    chosen = jax.random.randint(jax.random.fold_in(key, 22), (), 0, BUCKETS).astype(jnp.int32)
    single = jnp.concatenate([filled, jnp.zeros((BUCKETS, PER - 1), jnp.int32)], axis=1)
    rows = jnp.arange(BUCKETS, dtype=jnp.int32)[:, None] == chosen
    return jnp.where(rows, single, lengths).astype(jnp.int32)


def level_of(stream_key, shape, shards, smallest, largest):
    def one(dim, parts):
        draws = jax.random.uniform(jax.random.fold_in(jax.random.fold_in(stream_key, 6), dim), (parts,), jnp.float32, smallest / len(shards), largest / len(shards))
        return jnp.repeat(jnp.exp(draws), shape[dim] // parts).reshape((-1,) + (1,) * (len(shape) - dim - 1))

    loudness = one(*shards[0])
    for cut in shards[1:]:
        loudness = loudness * one(*cut)
    return loudness


def noise(rng, extent, spread, limit, split=(), kind=jnp.bfloat16):
    drawn = jax.random.normal(rng, extent, jnp.float32) * spread
    if len(split) > 0:
        drawn = level_of(rng, extent, split, -0.22, 0.18) * drawn
    return jnp.clip(drawn, min=-limit, max=limit).astype(kind)


def setup_inputs(seed: int = 0) -> dict:
    key_list = jax.random.split(jax.random.key(seed), 5)
    return {
        "query": draw_query(jax.random.fold_in(key_list[4], 71), 0),
        "key": draw_key(jax.random.fold_in(key_list[4], 71), 0),
        "value": noise(key_list[2], (TOKENS, D), 1.0, 6.0, ((0, 16), (1, 2))),
        "clip_lengths": draw_clip_lengths(jax.random.fold_in(key_list[4], 71), 0),
    }


NEG = -1.0e30


def clip_of(places, ends):
    bucket = (places // MOST).astype(jnp.int32)
    offset = (places - bucket * MOST).astype(jnp.int32)
    hits = jnp.sum((offset[:, None, None] >= ends[None, :, :]).astype(jnp.int32), axis=2).astype(jnp.int32)
    pick = bucket[:, None] == jnp.arange(BUCKETS, dtype=jnp.int32)[None, :]
    inner = jnp.sum(jnp.where(pick, hits, 0), axis=1).astype(jnp.int32)
    return (bucket * PER + inner).astype(jnp.int32)


def reference(query, key, value, clip_lengths):
    heads = D // HD
    scale = 1.0 / (HD ** 0.5)
    ends = jnp.cumsum(clip_lengths, axis=1).astype(jnp.int32)
    clip_ids = clip_of(jnp.arange(TOKENS, dtype=jnp.int32), ends)
    block = min(512, MOST)
    outputs = []
    for bucket in range(BUCKETS):
        low = bucket * MOST
        k_part = key[low:low + MOST].reshape(MOST, heads, HD).astype(jnp.float32)
        v_part = value[low:low + MOST].reshape(MOST, heads, HD).astype(jnp.float32)
        k_ids = clip_ids[low:low + MOST]
        q_all = query[low:low + MOST].reshape(MOST // block, block, heads, HD)
        q_idx = k_ids.reshape(MOST // block, block)

        def one_block(items):
            q_part, q_ids = items
            score = jnp.einsum("qhd,khd->hqk", q_part.astype(jnp.float32), k_part,
                               precision=lax.Precision.HIGHEST) * scale
            keep = (q_ids[:, None] == k_ids[None, :])[None]
            score = jnp.where(keep, score, NEG)
            top = jnp.max(score, axis=-1, keepdims=True)
            weight = jnp.where(keep, jnp.exp(score - top), 0.0)
            total = jnp.sum(weight, axis=-1)
            weight_low = lax.optimization_barrier(weight.astype(jnp.bfloat16)).astype(jnp.float32)
            summed = jnp.einsum("hqk,khd->qhd", weight_low, v_part, precision=lax.Precision.HIGHEST)
            result = summed / jnp.transpose(total)[:, :, None]
            return result.reshape(block, D).astype(jnp.bfloat16)

        pieces = lax.map(one_block, (q_all, q_idx))
        outputs.append(pieces.reshape(MOST, D))
    return jnp.concatenate(outputs, axis=0)
```

```python
import functools

import jax
import jax.numpy as jnp
from jax import lax
from jax.experimental import pallas as pl
from jax.experimental.pallas import tpu as pltpu
from jax.sharding import PartitionSpec as P

HD = 128
NEG = -1e30
LOG2E = 1.4426950408889634
MESH = pl.DeviceIdType.MESH


def kernel(
    group, pair, mp, heads, lead,
    lengths, query, key, value, out,
    q_buf, k_buf, v_buf, o_buf, first, p_buf, t_buf,
    q_in, k_in, v_in, o_in, q_out, k_out, v_out, o_out, first_in, ready,
):
    rows = query.shape[0]
    part = rows // mp
    per_core = heads // pair
    others = group // pair
    extra = lead * (others - 1)
    held = per_core - extra
    slots = lengths.shape[1]
    seq_index = lax.axis_index("seq")
    mp_index = lax.axis_index("mp")
    bucket = seq_index // group
    place = lax.rem(seq_index, group)
    core = lax.rem(place, pair)
    chip = place // pair

    def chip_at(chip_step):
        return lax.rem(chip + chip_step, others)

    def seq_of(chip_step, there_core):
        return bucket * group + chip_at(chip_step) * pair + there_core

    def head_of(slot, there_chip):
        if isinstance(slot, int) and slot < lead:
            return slot * others + there_chip
        return slot + extra

    def columns(owner, head):
        return pl.ds(pl.multiple_of((owner * per_core + head) * HD, HD), HD)

    def block_at(index):
        return pl.ds(pl.multiple_of(index * rows, rows), rows)

    kinds = ((query, q_buf, q_out, q_in), (key, k_buf, k_out, k_in), (value, v_buf, v_out, v_in))

    def local_copies(slot):
        mine = columns(core, head_of(slot, chip))
        return [
            pltpu.make_async_copy(source.at[:, mine], buf.at[slot, block_at(place), :], landed.at[slot, place])
            for source, buf, left, landed in kinds
        ]

    def far_kinds(slot):
        whole = isinstance(slot, int) and slot < lead
        return (0, 1, 2) if whole else (1, 2)

    far = [(chip_step, there_core) for there_core in range(pair) for chip_step in range(1, others)]

    def first_copies():
        return [
            pltpu.make_async_copy(
                kinds[kind][0].at[:, columns(there_core, head_of(0, chip_at(chip_step)))],
                first.at[kind, chip_step * pair + there_core],
                first_in.at[kind, chip_step * pair + there_core],
            )
            for kind in far_kinds(0) for chip_step, there_core in far
        ]

    def send(slot, chip_step, there_core, kind, staged=False):
        source, buf, left, landed = kinds[kind]
        index = chip_step * pair + there_core
        if staged:
            origin = first.at[kind, index]
        else:
            origin = source.at[:, columns(there_core, head_of(slot, chip_at(chip_step)))]
        return pltpu.make_async_remote_copy(
            src_ref=origin, dst_ref=buf.at[slot, block_at(place), :],
            send_sem=left.at[slot, index], recv_sem=landed.at[slot, place],
            device_id={"seq": seq_of(chip_step, there_core), "mp": mp_index}, device_id_type=MESH,
        )

    def far_sends(slot, staged=False):
        return [send(slot, a, b, kind, staged) for kind in far_kinds(slot) for a, b in far]

    def near_sends(slot):
        return [
            send(slot, 0, lax.rem(core + step, pair), kind)
            for kind in range(3) for step in range(1, pair)
        ]

    def result(turn, slot, chip_step, core_step, mp_step):
        there_core = lax.rem(core + core_step, pair)
        there_mp = lax.rem(mp_index + mp_step, mp)
        source = o_buf.at[turn, pl.ds(pl.multiple_of(there_core * rows + there_mp * part, part), part), :]
        column = (mp_index * heads + core * per_core + head_of(slot, chip)) * HD
        target = out.at[:, pl.ds(pl.multiple_of(column, HD), HD)]
        index = core_step * mp + mp_step
        if chip_step == 0 and index == 0:
            return pltpu.make_async_copy(source, target, o_in.at[turn, index])
        return pltpu.make_async_remote_copy(
            src_ref=source, dst_ref=target, send_sem=o_out.at[turn, index], recv_sem=o_in.at[turn, index],
            device_id={"seq": seq_of(chip_step, there_core), "mp": there_mp}, device_id_type=MESH,
        )

    for copy in first_copies():
        copy.start()

    barrier = pltpu.get_barrier_semaphore()
    beside = [(seq_of(0, b), lax.rem(mp_index + m, mp)) for b in range(pair) for m in range(1, mp)]
    greeted = [(seq_of(a, b), mp_index) for a, b in far]
    greeted += [(seq_of(0, lax.rem(core + b, pair)), mp_index) for b in range(1, pair)]
    greeted += beside
    for there_seq, there_mp in greeted:
        pl.semaphore_signal(
            barrier, inc=1, device_id={"seq": there_seq, "mp": there_mp}, device_id_type=MESH
        )

    for slot in range(max(lead, 1)):
        for copy in local_copies(slot):
            copy.start()

    @pl.loop(max(lead, 1), held)
    def _(slot):
        for copy in local_copies(slot):
            copy.start()

    ends = []
    running = jnp.int32(0)
    for i in range(slots):
        running = running + lengths[bucket, i]
        ends.append(running)

    def ids(offset):
        found = jnp.zeros_like(offset)
        for end in ends:
            found = found + (offset >= end).astype(jnp.int32)
        return found

    k_ids = ids(lax.broadcasted_iota(jnp.int32, (1, group * rows), 1))

    for copy in first_copies():
        copy.wait()
    pl.semaphore_wait(barrier, len(greeted))

    for slot in range(max(lead, 1)):
        for copy in far_sends(slot, slot == 0) + near_sends(slot):
            copy.start()

    @pl.loop(max(lead, 1), held)
    def _(slot):
        for copy in far_sends(slot) + near_sends(slot):
            copy.start()

    if lead:
        for there_seq, there_mp in beside:
            pl.semaphore_signal(
                ready, inc=1, device_id={"seq": there_seq, "mp": there_mp}, device_id_type=MESH
            )

    def arrived(kind, slot, base, count):
        buf, landed = kinds[kind][1], kinds[kind][3]
        for i in range(count):
            ref = buf.at[slot, block_at(base + i), :]
            pltpu.make_async_copy(ref, ref, landed.at[slot, base + i]).wait()

    factor = LOG2E / HD**0.5

    def weigh(slot, chip_step):
        keys = k_buf[slot]
        for b in range(pair):
            block = pl.ds(b * rows, rows)
            from_row = (chip_at(chip_step) * pair + b) * rows
            q_ids = ids(lax.broadcasted_iota(jnp.int32, (rows, 1), 0) + from_row)
            score = lax.dot_general(
                q_buf[slot, pl.ds(pl.multiple_of(from_row, rows), rows), :], keys,
                (((1,), (1,)), ((), ())), preferred_element_type=jnp.float32,
            )
            score = jnp.where(q_ids == k_ids, score, NEG)
            top = jnp.max(score, axis=1, keepdims=True)
            weight = jnp.exp2((score - top) * factor)
            t_buf[block, :] = jnp.broadcast_to(jnp.sum(weight, axis=1, keepdims=True), (rows, HD))
            p_buf[block, :] = weight.astype(jnp.bfloat16)

    def attend(turn, slot, chip_step):
        for core_step in reversed(range(pair)):
            block = block_at(lax.rem(core + core_step, pair))
            summed = jnp.dot(p_buf[block, :], v_buf[slot], preferred_element_type=jnp.float32)
            o_buf[turn, block, :] = (summed / t_buf[block, :]).astype(jnp.bfloat16)
            if chip_step == 0:
                for mp_step in reversed(range(mp)):
                    result(turn, slot, 0, core_step, mp_step).start()

    def far_results(mp_steps):
        return [
            result(slot * (others - 1) + a - 1, slot, a, core_step, mp_step)
            for slot in range(lead) for mp_step in mp_steps
            for core_step in range(pair) for a in range(1, others)
        ]

    def settle(turn, slot, chip_step=0):
        for core_step in range(pair):
            for mp_step in range(mp):
                copy = result(turn, slot, chip_step, core_step, mp_step)
                if chip_step == 0 and core_step == 0 and mp_step == 0:
                    copy.wait()
                else:
                    copy.wait_send()
                    copy.wait_recv()

    for slot in range(lead):
        arrived(0, slot, 0, group)
        arrived(1, slot, 0, group)
        for step in range(1, others):
            weigh(slot, step)
            if step == 1:
                arrived(2, slot, 0, group)
            attend(slot * (others - 1) + step - 1, slot, step)
        weigh(slot, 0)
        attend(slot + extra, slot, 0)
        for copy in far_sends(slot, slot == 0) + near_sends(slot):
            copy.wait_send()
    if lead:
        pl.semaphore_wait(ready, len(beside))
        for copy in far_results(list(range(1, mp)) + [0]):
            copy.start()

    @pl.loop(lead, held)
    def _(slot):
        arrived(0, slot, chip * pair, pair)
        arrived(1, slot, 0, group)
        weigh(slot, 0)
        arrived(2, slot, 0, group)
        attend(slot + extra, slot, 0)
        for copy in far_sends(slot) + near_sends(slot):
            copy.wait_send()

        @pl.when(slot > lead)
        def _():
            settle(slot + extra - 1, slot - 1)

    for slot in range(lead):
        settle(slot + extra, slot)
    settle(held - 1 + extra, held - 1)
    for slot in range(lead):
        for step in range(1, others):
            settle(slot * (others - 1) + step - 1, slot, step)


def duo(
    heads,
    lengths, query, key, value, out,
    kept, weights, totals, results, table,
    landed, sent, result_in, result_out, table_in, ready,
):
    rows = query.shape[0]
    mp = lax.axis_size("mp")
    part = rows // mp
    per_core = heads // 2
    wide = per_core // 3
    width = wide * HD
    slots = lengths.shape[1]
    seq_index = lax.axis_index("seq")
    mp_index = lax.axis_index("mp")
    bucket = seq_index // 4
    place = lax.rem(seq_index, 4)
    core = lax.rem(place, 2)
    chip = place // 2
    other = 1 - chip
    inputs = (query, key, value)

    def device(there_chip, there_core, there_mp):
        return {"seq": bucket * 4 + there_chip * 2 + there_core, "mp": there_mp}

    def columns(owner, third):
        return pl.ds(pl.multiple_of(owner * per_core * HD + third * width, width), width)

    def block_at(index):
        return pl.ds(pl.multiple_of(index * rows, rows), rows)

    def send(kind, phase, there_chip, there_core):
        third = 2 if phase else there_chip
        return pltpu.make_async_remote_copy(
            src_ref=inputs[kind].at[:, columns(there_core, third)],
            dst_ref=kept.at[kind, phase, block_at(place), :],
            send_sem=sent, recv_sem=landed.at[kind, phase],
            device_id=device(there_chip, there_core, mp_index), device_id_type=MESH,
        )

    def keep(kind, phase):
        third = 2 if phase else chip
        return pltpu.make_async_copy(
            inputs[kind].at[:, columns(core, third)], kept.at[kind, phase, block_at(place), :], landed.at[kind, phase]
        )

    def result(turn, there_chip, core_step, mp_step):
        there_core = lax.rem(core + core_step, 2)
        there_mp = lax.rem(mp_index + mp_step, mp)
        first = (there_chip * 2 + there_core) * rows + there_mp * part
        source = results.at[turn, pl.ds(pl.multiple_of(first, part), part), :]
        third = 2 if turn else chip
        column = (mp_index * heads + core * per_core) * HD + third * width
        target = out.at[:, pl.ds(pl.multiple_of(column, width), width)]
        if there_chip is chip and core_step == 0 and mp_step == 0:
            target[...] = source[...]
            return
        pltpu.make_async_remote_copy(
            src_ref=source, dst_ref=target, send_sem=result_out, recv_sem=result_in,
            device_id=device(there_chip, there_core, there_mp), device_id_type=MESH,
        ).start()

    barrier = pltpu.get_barrier_semaphore()
    far = [device(other, b, mp_index) for b in range(2)]
    beside = [device(chip, b, lax.rem(mp_index + m, mp)) for m in range(1, mp) for b in range(2)]

    def greet(semaphore, devices):
        for there in devices:
            pl.semaphore_signal(semaphore, inc=1, device_id=there, device_id_type=MESH)

    greet(barrier, far)
    pl.when(chip == 0)(lambda: greet(barrier, beside))
    known = len(far) + lax.select(chip == 0, len(beside), 0)
    pl.semaphore_wait(barrier, known)

    for kind, phase in ((1, 0), (0, 0), (2, 0), (1, 1), (2, 1)):
        for there_core in range(2):
            send(kind, phase, other, there_core).start()
    fetch = pltpu.make_async_copy(lengths, table, table_in)
    fetch.start()
    for phase in range(2):
        for kind in (1, 0, 2):
            keep(kind, phase).start()

    greet(ready, far)

    @pl.when(chip == 0)
    def _():
        greet(ready, beside)
        pl.semaphore_wait(ready, len(far) + len(beside))
        greet(ready, far)

    pl.when(chip != 0)(lambda: pl.semaphore_wait(ready, 2 * len(far)))

    for phase in range(2):
        for kind in (1, 0, 2):
            send(kind, phase, chip, 1 - core).start()

    fetch.wait()
    ends = []
    running = jnp.int32(0)
    for i in range(slots):
        running = running + table[bucket, i]
        ends.append(running)

    def ids(offset):
        found = jnp.zeros_like(offset)
        for end in ends:
            found = found + (offset >= end).astype(jnp.int32)
        return found

    k_ids = ids(lax.broadcasted_iota(jnp.int32, (1, 4 * rows), 1))
    factor = LOG2E / HD**0.5

    def arrived(kind, phase):
        ref = kept.at[kind, phase]
        if kind == 0 and phase:
            ref = kept.at[kind, phase, pl.ds(pl.multiple_of(chip * 2 * rows, rows), 2 * rows), :]
        pltpu.make_async_copy(ref, ref, landed.at[kind, phase]).wait()

    def weigh(phase, index):
        block = block_at(index)
        q_ids = ids(lax.broadcasted_iota(jnp.int32, (rows, 1), 0) + index * rows)
        for head in range(wide):
            lanes = slice(head * HD, (head + 1) * HD)
            score = lax.dot_general(
                kept[0, phase, block, lanes], kept[1, phase, :, lanes],
                (((1,), (1,)), ((), ())), preferred_element_type=jnp.float32,
            )
            score = jnp.where(q_ids == k_ids, score, NEG)
            top = jnp.max(score, axis=1, keepdims=True)
            weight = jnp.exp2((score - top) * factor)
            totals[head, block, :] = jnp.broadcast_to(jnp.sum(weight, axis=1, keepdims=True), (rows, HD))
            weights[head, block, :] = weight.astype(jnp.bfloat16)

    def attend(phase, index):
        block = block_at(index)
        for head in range(wide):
            lanes = slice(head * HD, (head + 1) * HD)
            summed = jnp.dot(weights[head, block, :], kept[2, phase, :, lanes], preferred_element_type=jnp.float32)
            results[phase, block, lanes] = (summed / totals[head, block, :]).astype(jnp.bfloat16)

    arrived(1, 0)
    arrived(0, 0)

    @pl.loop(0, 4)
    def _(step):
        weigh(0, lax.rem(other * 2 + step, 4))

    arrived(2, 0)

    @pl.loop(0, 4)
    def _(step):
        attend(0, lax.rem(other * 2 + step, 4))

    for core_step in range(2):
        result(0, other, core_step, 0)
    for core_step in reversed(range(2)):
        for mp_step in reversed(range(mp)):
            result(0, chip, core_step, mp_step)

    arrived(1, 1)
    arrived(0, 1)

    @pl.loop(0, 2)
    def _(step):
        weigh(1, chip * 2 + step)

    for mp_step in range(1, mp):
        for core_step in range(2):
            result(0, other, core_step, mp_step)

    arrived(2, 1)
    for core_step in reversed(range(2)):
        attend(1, chip * 2 + lax.rem(core + core_step, 2))
        for mp_step in reversed(range(mp)):
            result(1, chip, core_step, mp_step)

    whole = kept.at[pl.ds(0, 2)]
    pltpu.make_async_copy(whole, whole, sent).wait()
    moved = out.at[:, pl.ds(0, out.shape[1] - 2 * width)]
    pltpu.make_async_copy(moved, moved, result_out).wait()
    pltpu.make_async_copy(moved, moved, result_in).wait()


def duo_call(query, key, value, clip_lengths):
    rows, width = query.shape
    heads = width // HD
    mp = lax.axis_size("mp")
    wide = heads // 6
    dma = pltpu.SemaphoreType.DMA
    whole = pl.BlockSpec(memory_space=pl.ANY)
    return pl.pallas_call(
        functools.partial(duo, heads),
        out_shape=pltpu.VMEM((rows // mp, width * mp), jnp.bfloat16),
        in_specs=[whole] * 4,
        out_specs=pl.BlockSpec(memory_space=pltpu.VMEM),
        scratch_shapes=[
            pltpu.VMEM((3, 2, 4 * rows, wide * HD), jnp.bfloat16),
            pltpu.VMEM((wide, 4 * rows, 4 * rows), jnp.bfloat16),
            pltpu.VMEM((wide, 4 * rows, HD), jnp.float32),
            pltpu.VMEM((2, 4 * rows, wide * HD), jnp.bfloat16),
            pltpu.SMEM(clip_lengths.shape, jnp.int32),
            dma((3, 2)), dma(()), dma(()), dma(()), dma(()), pltpu.SemaphoreType.REGULAR,
        ],
        compiler_params=pltpu.CompilerParams(collective_id=0, has_side_effects=True),
        name="packed_attention",
    )(clip_lengths, query, key, value)


def shards(query, key, value, clip_lengths):
    rows, width = query.shape
    heads = width // HD
    group = lax.axis_size("seq") // clip_lengths.shape[0]
    mp = lax.axis_size("mp")
    if group == 4 and heads % 6 == 0 and rows % (16 * mp) == 0 and 1 < mp:
        return duo_call(query, key, value, clip_lengths)
    pair = 2 if group % 2 == 0 and heads % 2 == 0 else 1
    per_core = heads // pair
    others = group // pair
    lead = min(2, (per_core - 1) // others) if others > 1 else 0
    held = per_core - lead * (others - 1)
    dma = pltpu.SemaphoreType.DMA
    whole = pl.BlockSpec(memory_space=pl.ANY)
    return pl.pallas_call(
        functools.partial(kernel, group, pair, mp, heads, lead),
        out_shape=pltpu.VMEM((rows // mp, width * mp), jnp.bfloat16),
        in_specs=[pl.BlockSpec(memory_space=pltpu.SMEM), whole, whole, whole],
        out_specs=pl.BlockSpec(memory_space=pltpu.VMEM),
        scratch_shapes=[
            pltpu.VMEM((held, group * rows, HD), jnp.bfloat16),
            pltpu.VMEM((held, group * rows, HD), jnp.bfloat16),
            pltpu.VMEM((held, group * rows, HD), jnp.bfloat16),
            pltpu.VMEM((per_core, pair * rows, HD), jnp.bfloat16),
            pltpu.VMEM((3, group, rows, HD), jnp.bfloat16),
            pltpu.VMEM((pair * rows, group * rows), jnp.bfloat16),
            pltpu.VMEM((pair * rows, HD), jnp.float32),
            dma((held, group)), dma((held, group)), dma((held, group)), dma((per_core, pair * mp)),
            dma((held, group)), dma((held, group)), dma((held, group)), dma((per_core, pair * mp)),
            dma((3, group)), pltpu.SemaphoreType.REGULAR,
        ],
        compiler_params=pltpu.CompilerParams(collective_id=0, has_side_effects=True),
        name="packed_attention",
    )(clip_lengths, query, key, value)


def solution(mesh):
    in_specs = (P("seq", "mp"), P("seq", "mp"), P("seq", "mp"), P())
    out_specs = P(("seq", "mp"), None)
    return jax.shard_map(shards, mesh=mesh, in_specs=in_specs, out_specs=out_specs, check_vma=False)
```

```python
import functools

import jax
import jax.numpy as jnp
from jax import lax
from jax.experimental import pallas as pl
from jax.experimental.pallas import tpu as pltpu
from jax.sharding import PartitionSpec as P

HD = 128
NEG = -1e30
LOG2E = 1.4426950408889634
MESH = pl.DeviceIdType.MESH


def kernel(
    group, pair, mp, heads, lead,
    lengths, query, key, value, out,
    q_buf, k_buf, v_buf, o_buf, first, p_buf, t_buf,
    q_in, k_in, v_in, o_in, q_out, k_out, v_out, o_out, first_in, ready,
):
    rows = query.shape[0]
    part = rows // mp
    per_core = heads // pair
    others = group // pair
    extra = lead * (others - 1)
    held = per_core - extra
    slots = lengths.shape[1]
    seq_index = lax.axis_index("seq")
    mp_index = lax.axis_index("mp")
    bucket = seq_index // group
    place = lax.rem(seq_index, group)
    core = lax.rem(place, pair)
    chip = place // pair

    def chip_at(chip_step):
        return lax.rem(chip + chip_step, others)

    def seq_of(chip_step, there_core):
        return bucket * group + chip_at(chip_step) * pair + there_core

    def head_of(slot, there_chip):
        if isinstance(slot, int) and slot < lead:
            return slot * others + there_chip
        return slot + extra

    def columns(owner, head):
        return pl.ds(pl.multiple_of((owner * per_core + head) * HD, HD), HD)

    def block_at(index):
        return pl.ds(pl.multiple_of(index * rows, rows), rows)

    kinds = ((query, q_buf, q_out, q_in), (key, k_buf, k_out, k_in), (value, v_buf, v_out, v_in))

    def local_copies(slot):
        mine = columns(core, head_of(slot, chip))
        return [
            pltpu.make_async_copy(source.at[:, mine], buf.at[slot, block_at(place), :], landed.at[slot, place])
            for source, buf, left, landed in kinds
        ]

    def far_kinds(slot):
        whole = isinstance(slot, int) and slot < lead
        return (0, 1, 2) if whole else (1, 2)

    far = [(chip_step, there_core) for there_core in range(pair) for chip_step in range(1, others)]

    def first_copies():
        return [
            pltpu.make_async_copy(
                kinds[kind][0].at[:, columns(there_core, head_of(0, chip_at(chip_step)))],
                first.at[kind, chip_step * pair + there_core],
                first_in.at[kind, chip_step * pair + there_core],
            )
            for kind in far_kinds(0) for chip_step, there_core in far
        ]

    def send(slot, chip_step, there_core, kind, staged=False):
        source, buf, left, landed = kinds[kind]
        index = chip_step * pair + there_core
        if staged:
            origin = first.at[kind, index]
        else:
            origin = source.at[:, columns(there_core, head_of(slot, chip_at(chip_step)))]
        return pltpu.make_async_remote_copy(
            src_ref=origin, dst_ref=buf.at[slot, block_at(place), :],
            send_sem=left.at[slot, index], recv_sem=landed.at[slot, place],
            device_id={"seq": seq_of(chip_step, there_core), "mp": mp_index}, device_id_type=MESH,
        )

    def far_sends(slot, staged=False):
        return [send(slot, a, b, kind, staged) for kind in far_kinds(slot) for a, b in far]

    def near_sends(slot):
        return [
            send(slot, 0, lax.rem(core + step, pair), kind)
            for kind in range(3) for step in range(1, pair)
        ]

    def result(turn, slot, chip_step, core_step, mp_step):
        there_core = lax.rem(core + core_step, pair)
        there_mp = lax.rem(mp_index + mp_step, mp)
        source = o_buf.at[turn, pl.ds(pl.multiple_of(there_core * rows + there_mp * part, part), part), :]
        column = (mp_index * heads + core * per_core + head_of(slot, chip)) * HD
        target = out.at[:, pl.ds(pl.multiple_of(column, HD), HD)]
        index = core_step * mp + mp_step
        if chip_step == 0 and index == 0:
            return pltpu.make_async_copy(source, target, o_in.at[turn, index])
        return pltpu.make_async_remote_copy(
            src_ref=source, dst_ref=target, send_sem=o_out.at[turn, index], recv_sem=o_in.at[turn, index],
            device_id={"seq": seq_of(chip_step, there_core), "mp": there_mp}, device_id_type=MESH,
        )

    for copy in first_copies():
        copy.start()

    barrier = pltpu.get_barrier_semaphore()
    beside = [(seq_of(0, b), lax.rem(mp_index + m, mp)) for b in range(pair) for m in range(1, mp)]
    greeted = [(seq_of(a, b), mp_index) for a, b in far]
    greeted += [(seq_of(0, lax.rem(core + b, pair)), mp_index) for b in range(1, pair)]
    greeted += beside
    for there_seq, there_mp in greeted:
        pl.semaphore_signal(
            barrier, inc=1, device_id={"seq": there_seq, "mp": there_mp}, device_id_type=MESH
        )

    for slot in range(max(lead, 1)):
        for copy in local_copies(slot):
            copy.start()

    @pl.loop(max(lead, 1), held)
    def _(slot):
        for copy in local_copies(slot):
            copy.start()

    ends = []
    running = jnp.int32(0)
    for i in range(slots):
        running = running + lengths[bucket, i]
        ends.append(running)

    def ids(offset):
        found = jnp.zeros_like(offset)
        for end in ends:
            found = found + (offset >= end).astype(jnp.int32)
        return found

    k_ids = ids(lax.broadcasted_iota(jnp.int32, (1, group * rows), 1))

    for copy in first_copies():
        copy.wait()
    pl.semaphore_wait(barrier, len(greeted))

    for slot in range(max(lead, 1)):
        for copy in far_sends(slot, slot == 0) + near_sends(slot):
            copy.start()

    @pl.loop(max(lead, 1), held)
    def _(slot):
        for copy in far_sends(slot) + near_sends(slot):
            copy.start()

    if lead:
        for there_seq, there_mp in beside:
            pl.semaphore_signal(
                ready, inc=1, device_id={"seq": there_seq, "mp": there_mp}, device_id_type=MESH
            )

    def arrived(kind, slot, base, count):
        buf, landed = kinds[kind][1], kinds[kind][3]
        for i in range(count):
            ref = buf.at[slot, block_at(base + i), :]
            pltpu.make_async_copy(ref, ref, landed.at[slot, base + i]).wait()

    factor = LOG2E / HD**0.5

    def weigh(slot, chip_step):
        keys = k_buf[slot]
        for b in range(pair):
            block = pl.ds(b * rows, rows)
            from_row = (chip_at(chip_step) * pair + b) * rows
            q_ids = ids(lax.broadcasted_iota(jnp.int32, (rows, 1), 0) + from_row)
            score = lax.dot_general(
                q_buf[slot, pl.ds(pl.multiple_of(from_row, rows), rows), :], keys,
                (((1,), (1,)), ((), ())), preferred_element_type=jnp.float32,
            )
            score = jnp.where(q_ids == k_ids, score, NEG)
            top = jnp.max(score, axis=1, keepdims=True)
            weight = jnp.exp2((score - top) * factor)
            t_buf[block, :] = jnp.broadcast_to(jnp.sum(weight, axis=1, keepdims=True), (rows, HD))
            p_buf[block, :] = weight.astype(jnp.bfloat16)

    def attend(turn, slot, chip_step):
        for core_step in reversed(range(pair)):
            block = block_at(lax.rem(core + core_step, pair))
            summed = jnp.dot(p_buf[block, :], v_buf[slot], preferred_element_type=jnp.float32)
            o_buf[turn, block, :] = (summed / t_buf[block, :]).astype(jnp.bfloat16)
            if chip_step == 0:
                for mp_step in reversed(range(mp)):
                    result(turn, slot, 0, core_step, mp_step).start()

    def far_results(mp_steps):
        return [
            result(slot * (others - 1) + a - 1, slot, a, core_step, mp_step)
            for slot in range(lead) for mp_step in mp_steps
            for core_step in range(pair) for a in range(1, others)
        ]

    def settle(turn, slot, chip_step=0):
        for core_step in range(pair):
            for mp_step in range(mp):
                copy = result(turn, slot, chip_step, core_step, mp_step)
                if chip_step == 0 and core_step == 0 and mp_step == 0:
                    copy.wait()
                else:
                    copy.wait_send()
                    copy.wait_recv()

    for slot in range(lead):
        arrived(0, slot, 0, group)
        arrived(1, slot, 0, group)
        for step in range(1, others):
            weigh(slot, step)
            if step == 1:
                arrived(2, slot, 0, group)
            attend(slot * (others - 1) + step - 1, slot, step)
        weigh(slot, 0)
        attend(slot + extra, slot, 0)
        for copy in far_sends(slot, slot == 0) + near_sends(slot):
            copy.wait_send()
    if lead:
        pl.semaphore_wait(ready, len(beside))
        for copy in far_results(list(range(1, mp)) + [0]):
            copy.start()

    @pl.loop(lead, held)
    def _(slot):
        arrived(0, slot, chip * pair, pair)
        arrived(1, slot, 0, group)
        weigh(slot, 0)
        arrived(2, slot, 0, group)
        attend(slot + extra, slot, 0)
        for copy in far_sends(slot) + near_sends(slot):
            copy.wait_send()

        @pl.when(slot > lead)
        def _():
            settle(slot + extra - 1, slot - 1)

    for slot in range(lead):
        settle(slot + extra, slot)
    settle(held - 1 + extra, held - 1)
    for slot in range(lead):
        for step in range(1, others):
            settle(slot * (others - 1) + step - 1, slot, step)


def duo(
    heads, pieces,
    lengths, query, key, value, out,
    kept, weights, totals, results, table,
    landed, sent, result_in, result_out, table_in, ready,
):
    rows = query.shape[0]
    mp = lax.axis_size("mp")
    part = rows // mp
    wide = heads // 4
    slots = lengths.shape[1]
    seq_index = lax.axis_index("seq")
    mp_index = lax.axis_index("mp")
    bucket = seq_index // 4
    place = lax.rem(seq_index, 4)
    core = lax.rem(place, 2)
    chip = place // 2
    other = 1 - chip
    inputs = (query, key, value)

    def device(there_chip, there_core, there_mp):
        return {"seq": bucket * 4 + there_chip * 2 + there_core, "mp": there_mp}

    def lanes(piece, base=0):
        first, count = pieces[piece]
        return pl.ds(pl.multiple_of((base + first) * HD, HD), count * HD)

    def block_at(index):
        return pl.ds(pl.multiple_of(index * rows, rows), rows)

    def send(kind, piece, there_chip, there_core):
        return pltpu.make_async_remote_copy(
            src_ref=inputs[kind].at[:, lanes(piece, (there_core * 2 + there_chip) * wide)],
            dst_ref=kept.at[kind, block_at(place), lanes(piece)],
            send_sem=sent, recv_sem=landed.at[kind, piece],
            device_id=device(there_chip, there_core, mp_index), device_id_type=MESH,
        )

    def keep(kind, piece):
        return pltpu.make_async_copy(
            inputs[kind].at[:, lanes(piece, (core * 2 + chip) * wide)],
            kept.at[kind, block_at(place), lanes(piece)], landed.at[kind, piece],
        )

    def result(piece, there_chip, core_step, mp_step):
        there_core = lax.rem(core + core_step, 2)
        there_mp = lax.rem(mp_index + mp_step, mp)
        first = (there_chip * 2 + there_core) * rows + there_mp * part
        source = results.at[pl.ds(pl.multiple_of(first, part), part), lanes(piece)]
        target = out.at[:, lanes(piece, mp_index * heads + (core * 2 + chip) * wide)]
        if there_chip is chip and core_step == 0 and mp_step == 0:
            target[...] = source[...]
            return
        pltpu.make_async_remote_copy(
            src_ref=source, dst_ref=target, send_sem=result_out, recv_sem=result_in,
            device_id=device(there_chip, there_core, there_mp), device_id_type=MESH,
        ).start()

    barrier = pltpu.get_barrier_semaphore()
    far = [device(other, b, mp_index) for b in range(2)]
    beside = [device(chip, b, lax.rem(mp_index + m, mp)) for m in range(1, mp) for b in range(2)]

    def greet(semaphore, devices):
        for there in devices:
            pl.semaphore_signal(semaphore, inc=1, device_id=there, device_id_type=MESH)

    greet(barrier, far)
    pl.when(chip == 0)(lambda: greet(barrier, beside))
    known = len(far) + lax.select(chip == 0, len(beside), 0)
    pl.semaphore_wait(barrier, known)

    for piece in range(len(pieces)):
        for kind in (1, 0, 2):
            for there_core in range(2):
                send(kind, piece, other, there_core).start()
    fetch = pltpu.make_async_copy(lengths, table, table_in)
    fetch.start()
    for piece in range(len(pieces)):
        for kind in (1, 0, 2):
            keep(kind, piece).start()

    greet(ready, far)

    @pl.when(chip == 0)
    def _():
        greet(ready, beside)
        pl.semaphore_wait(ready, len(far) + len(beside))
        greet(ready, far)

    pl.when(chip != 0)(lambda: pl.semaphore_wait(ready, 2 * len(far)))

    for piece in range(len(pieces)):
        for kind in (1, 0, 2):
            send(kind, piece, chip, 1 - core).start()

    fetch.wait()
    ends = []
    running = jnp.int32(0)
    for i in range(slots):
        running = running + table[bucket, i]
        ends.append(running)

    def ids(offset):
        found = jnp.zeros_like(offset)
        for end in ends:
            found = found + (offset >= end).astype(jnp.int32)
        return found

    k_ids = ids(lax.broadcasted_iota(jnp.int32, (1, 4 * rows), 1))
    factor = LOG2E / HD**0.5

    def arrived(kind, piece):
        ref = kept.at[kind, :, lanes(piece)]
        pltpu.make_async_copy(ref, ref, landed.at[kind, piece]).wait()

    def heads_of(piece):
        first, count = pieces[piece]
        return [(head, slice(head * HD, (head + 1) * HD)) for head in range(first, first + count)]

    def weigh(piece, index):
        block = block_at(index)
        q_ids = ids(lax.broadcasted_iota(jnp.int32, (rows, 1), 0) + index * rows)
        for head, lane in heads_of(piece):
            score = lax.dot_general(
                kept[0, block, lane], kept[1, :, lane],
                (((1,), (1,)), ((), ())), preferred_element_type=jnp.float32,
            )
            score = jnp.where(q_ids == k_ids, score, NEG)
            top = jnp.max(score, axis=1, keepdims=True)
            weight = jnp.exp2((score - top) * factor)
            totals[head, block, :] = jnp.broadcast_to(jnp.sum(weight, axis=1, keepdims=True), (rows, HD))
            weights[head, block, :] = weight.astype(jnp.bfloat16)

    def attend(piece, index):
        block = block_at(index)
        for head, lane in heads_of(piece):
            summed = jnp.dot(weights[head, block, :], kept[2, :, lane], preferred_element_type=jnp.float32)
            results[block, lane] = (summed / totals[head, block, :]).astype(jnp.bfloat16)

    def direct(piece):
        for core_step in range(2):
            result(piece, other, core_step, 0)

    def diagonal(piece):
        for mp_step in range(1, mp):
            for core_step in range(2):
                result(piece, other, core_step, mp_step)

    def own(piece):
        for core_step in reversed(range(2)):
            for mp_step in reversed(range(mp)):
                result(piece, chip, core_step, mp_step)

    for piece in range(len(pieces)):
        last = piece == len(pieces) - 1
        arrived(1, piece)
        arrived(0, piece)

        @pl.loop(0, 4)
        def _(step):
            weigh(piece, lax.rem(other * 2 + step, 4))

        arrived(2, piece)
        if last:
            diagonal(piece - 1)

        @pl.loop(0, 2)
        def _(step):
            attend(piece, other * 2 + step)

        if last:
            diagonal(piece)
        direct(piece)

        @pl.loop(0, 2)
        def _(step):
            attend(piece, chip * 2 + step)

        own(piece)

    whole = kept.at[:, pl.ds(0, 3 * rows)]
    pltpu.make_async_copy(whole, whole, sent).wait()
    moved = out.at[:, pl.ds(0, out.shape[1] - wide * HD)]
    pltpu.make_async_copy(moved, moved, result_out).wait()
    pltpu.make_async_copy(moved, moved, result_in).wait()


def duo_call(query, key, value, clip_lengths):
    rows, width = query.shape
    heads = width // HD
    mp = lax.axis_size("mp")
    wide = heads // 4
    early = (wide + 1) // 2
    pieces = [(0, early)] + [(head, 1) for head in range(early, wide)]
    dma = pltpu.SemaphoreType.DMA
    whole = pl.BlockSpec(memory_space=pl.ANY)
    return pl.pallas_call(
        functools.partial(duo, heads, pieces),
        out_shape=pltpu.VMEM((rows // mp, width * mp), jnp.bfloat16),
        in_specs=[whole] * 4,
        out_specs=pl.BlockSpec(memory_space=pltpu.VMEM),
        scratch_shapes=[
            pltpu.VMEM((3, 4 * rows, wide * HD), jnp.bfloat16),
            pltpu.VMEM((wide, 4 * rows, 4 * rows), jnp.bfloat16),
            pltpu.VMEM((wide, 4 * rows, HD), jnp.float32),
            pltpu.VMEM((4 * rows, wide * HD), jnp.bfloat16),
            pltpu.SMEM(clip_lengths.shape, jnp.int32),
            dma((3, len(pieces))), dma(()), dma(()), dma(()), dma(()), pltpu.SemaphoreType.REGULAR,
        ],
        compiler_params=pltpu.CompilerParams(collective_id=0, has_side_effects=True),
        name="packed_attention",
    )(clip_lengths, query, key, value)


def shards(query, key, value, clip_lengths):
    rows, width = query.shape
    heads = width // HD
    group = lax.axis_size("seq") // clip_lengths.shape[0]
    mp = lax.axis_size("mp")
    if group == 4 and heads % 4 == 0 and rows % (16 * mp) == 0 and mp > 1:
        return duo_call(query, key, value, clip_lengths)
    pair = 2 if group % 2 == 0 and heads % 2 == 0 else 1
    per_core = heads // pair
    others = group // pair
    lead = min(2, (per_core - 1) // others) if others > 1 else 0
    held = per_core - lead * (others - 1)
    dma = pltpu.SemaphoreType.DMA
    whole = pl.BlockSpec(memory_space=pl.ANY)
    return pl.pallas_call(
        functools.partial(kernel, group, pair, mp, heads, lead),
        out_shape=pltpu.VMEM((rows // mp, width * mp), jnp.bfloat16),
        in_specs=[pl.BlockSpec(memory_space=pltpu.SMEM), whole, whole, whole],
        out_specs=pl.BlockSpec(memory_space=pltpu.VMEM),
        scratch_shapes=[
            pltpu.VMEM((held, group * rows, HD), jnp.bfloat16),
            pltpu.VMEM((held, group * rows, HD), jnp.bfloat16),
            pltpu.VMEM((held, group * rows, HD), jnp.bfloat16),
            pltpu.VMEM((per_core, pair * rows, HD), jnp.bfloat16),
            pltpu.VMEM((3, group, rows, HD), jnp.bfloat16),
            pltpu.VMEM((pair * rows, group * rows), jnp.bfloat16),
            pltpu.VMEM((pair * rows, HD), jnp.float32),
            dma((held, group)), dma((held, group)), dma((held, group)), dma((per_core, pair * mp)),
            dma((held, group)), dma((held, group)), dma((held, group)), dma((per_core, pair * mp)),
            dma((3, group)), pltpu.SemaphoreType.REGULAR,
        ],
        compiler_params=pltpu.CompilerParams(collective_id=0, has_side_effects=True),
        name="packed_attention",
    )(clip_lengths, query, key, value)


def solution(mesh):
    in_specs = (P("seq", "mp"), P("seq", "mp"), P("seq", "mp"), P())
    out_specs = P(("seq", "mp"), None)
    return jax.shard_map(shards, mesh=mesh, in_specs=in_specs, out_specs=out_specs, check_vma=False)
```

```python
import functools

import jax
import jax.numpy as jnp
from jax import lax
from jax.experimental import pallas as pl
from jax.experimental.pallas import tpu as pltpu
from jax.sharding import PartitionSpec as P

HD = 128
NEG = -1e30
LOG2E = 1.4426950408889634
MESH = pl.DeviceIdType.MESH


def kernel(
    group, pair, mp, heads, lead,
    lengths, query, key, value, out,
    q_buf, k_buf, v_buf, o_buf, first, p_buf, t_buf,
    q_in, k_in, v_in, o_in, q_out, k_out, v_out, o_out, first_in, ready,
):
    rows = query.shape[0]
    part = rows // mp
    per_core = heads // pair
    others = group // pair
    extra = lead * (others - 1)
    held = per_core - extra
    slots = lengths.shape[1]
    seq_index = lax.axis_index("seq")
    mp_index = lax.axis_index("mp")
    bucket = seq_index // group
    place = lax.rem(seq_index, group)
    core = lax.rem(place, pair)
    chip = place // pair

    def chip_at(chip_step):
        return lax.rem(chip + chip_step, others)

    def seq_of(chip_step, there_core):
        return bucket * group + chip_at(chip_step) * pair + there_core

    def head_of(slot, there_chip):
        if isinstance(slot, int) and slot < lead:
            return slot * others + there_chip
        return slot + extra

    def columns(owner, head):
        return pl.ds(pl.multiple_of((owner * per_core + head) * HD, HD), HD)

    def block_at(index):
        return pl.ds(pl.multiple_of(index * rows, rows), rows)

    kinds = ((query, q_buf, q_out, q_in), (key, k_buf, k_out, k_in), (value, v_buf, v_out, v_in))

    def local_copies(slot):
        mine = columns(core, head_of(slot, chip))
        return [
            pltpu.make_async_copy(source.at[:, mine], buf.at[slot, block_at(place), :], landed.at[slot, place])
            for source, buf, left, landed in kinds
        ]

    def far_kinds(slot):
        whole = isinstance(slot, int) and slot < lead
        return (0, 1, 2) if whole else (1, 2)

    far = [(chip_step, there_core) for there_core in range(pair) for chip_step in range(1, others)]

    def first_copies():
        return [
            pltpu.make_async_copy(
                kinds[kind][0].at[:, columns(there_core, head_of(0, chip_at(chip_step)))],
                first.at[kind, chip_step * pair + there_core],
                first_in.at[kind, chip_step * pair + there_core],
            )
            for kind in far_kinds(0) for chip_step, there_core in far
        ]

    def send(slot, chip_step, there_core, kind, staged=False):
        source, buf, left, landed = kinds[kind]
        index = chip_step * pair + there_core
        if staged:
            origin = first.at[kind, index]
        else:
            origin = source.at[:, columns(there_core, head_of(slot, chip_at(chip_step)))]
        return pltpu.make_async_remote_copy(
            src_ref=origin, dst_ref=buf.at[slot, block_at(place), :],
            send_sem=left.at[slot, index], recv_sem=landed.at[slot, place],
            device_id={"seq": seq_of(chip_step, there_core), "mp": mp_index}, device_id_type=MESH,
        )

    def far_sends(slot, staged=False):
        return [send(slot, a, b, kind, staged) for kind in far_kinds(slot) for a, b in far]

    def near_sends(slot):
        return [
            send(slot, 0, lax.rem(core + step, pair), kind)
            for kind in range(3) for step in range(1, pair)
        ]

    def result(turn, slot, chip_step, core_step, mp_step):
        there_core = lax.rem(core + core_step, pair)
        there_mp = lax.rem(mp_index + mp_step, mp)
        source = o_buf.at[turn, pl.ds(pl.multiple_of(there_core * rows + there_mp * part, part), part), :]
        column = (mp_index * heads + core * per_core + head_of(slot, chip)) * HD
        target = out.at[:, pl.ds(pl.multiple_of(column, HD), HD)]
        index = core_step * mp + mp_step
        if chip_step == 0 and index == 0:
            return pltpu.make_async_copy(source, target, o_in.at[turn, index])
        return pltpu.make_async_remote_copy(
            src_ref=source, dst_ref=target, send_sem=o_out.at[turn, index], recv_sem=o_in.at[turn, index],
            device_id={"seq": seq_of(chip_step, there_core), "mp": there_mp}, device_id_type=MESH,
        )

    for copy in first_copies():
        copy.start()

    barrier = pltpu.get_barrier_semaphore()
    beside = [(seq_of(0, b), lax.rem(mp_index + m, mp)) for b in range(pair) for m in range(1, mp)]
    greeted = [(seq_of(a, b), mp_index) for a, b in far]
    greeted += [(seq_of(0, lax.rem(core + b, pair)), mp_index) for b in range(1, pair)]
    greeted += beside
    for there_seq, there_mp in greeted:
        pl.semaphore_signal(
            barrier, inc=1, device_id={"seq": there_seq, "mp": there_mp}, device_id_type=MESH
        )

    for slot in range(max(lead, 1)):
        for copy in local_copies(slot):
            copy.start()

    @pl.loop(max(lead, 1), held)
    def _(slot):
        for copy in local_copies(slot):
            copy.start()

    ends = []
    running = jnp.int32(0)
    for i in range(slots):
        running = running + lengths[bucket, i]
        ends.append(running)

    def ids(offset):
        found = jnp.zeros_like(offset)
        for end in ends:
            found = found + (offset >= end).astype(jnp.int32)
        return found

    k_ids = ids(lax.broadcasted_iota(jnp.int32, (1, group * rows), 1))

    for copy in first_copies():
        copy.wait()
    pl.semaphore_wait(barrier, len(greeted))

    for slot in range(max(lead, 1)):
        for copy in far_sends(slot, slot == 0) + near_sends(slot):
            copy.start()

    @pl.loop(max(lead, 1), held)
    def _(slot):
        for copy in far_sends(slot) + near_sends(slot):
            copy.start()

    if lead:
        for there_seq, there_mp in beside:
            pl.semaphore_signal(
                ready, inc=1, device_id={"seq": there_seq, "mp": there_mp}, device_id_type=MESH
            )

    def arrived(kind, slot, base, count):
        buf, landed = kinds[kind][1], kinds[kind][3]
        for i in range(count):
            ref = buf.at[slot, block_at(base + i), :]
            pltpu.make_async_copy(ref, ref, landed.at[slot, base + i]).wait()

    factor = LOG2E / HD**0.5

    def weigh(slot, chip_step):
        keys = k_buf[slot]
        for b in range(pair):
            block = pl.ds(b * rows, rows)
            from_row = (chip_at(chip_step) * pair + b) * rows
            q_ids = ids(lax.broadcasted_iota(jnp.int32, (rows, 1), 0) + from_row)
            score = lax.dot_general(
                q_buf[slot, pl.ds(pl.multiple_of(from_row, rows), rows), :], keys,
                (((1,), (1,)), ((), ())), preferred_element_type=jnp.float32,
            )
            score = jnp.where(q_ids == k_ids, score, NEG)
            top = jnp.max(score, axis=1, keepdims=True)
            weight = jnp.exp2((score - top) * factor)
            t_buf[block, :] = jnp.broadcast_to(jnp.sum(weight, axis=1, keepdims=True), (rows, HD))
            p_buf[block, :] = weight.astype(jnp.bfloat16)

    def attend(turn, slot, chip_step):
        for core_step in reversed(range(pair)):
            block = block_at(lax.rem(core + core_step, pair))
            summed = jnp.dot(p_buf[block, :], v_buf[slot], preferred_element_type=jnp.float32)
            o_buf[turn, block, :] = (summed / t_buf[block, :]).astype(jnp.bfloat16)
            if chip_step == 0:
                for mp_step in reversed(range(mp)):
                    result(turn, slot, 0, core_step, mp_step).start()

    def far_results(mp_steps):
        return [
            result(slot * (others - 1) + a - 1, slot, a, core_step, mp_step)
            for slot in range(lead) for mp_step in mp_steps
            for core_step in range(pair) for a in range(1, others)
        ]

    def settle(turn, slot, chip_step=0):
        for core_step in range(pair):
            for mp_step in range(mp):
                copy = result(turn, slot, chip_step, core_step, mp_step)
                if chip_step == 0 and core_step == 0 and mp_step == 0:
                    copy.wait()
                else:
                    copy.wait_send()
                    copy.wait_recv()

    for slot in range(lead):
        arrived(0, slot, 0, group)
        arrived(1, slot, 0, group)
        for step in range(1, others):
            weigh(slot, step)
            if step == 1:
                arrived(2, slot, 0, group)
            attend(slot * (others - 1) + step - 1, slot, step)
        weigh(slot, 0)
        attend(slot + extra, slot, 0)
        for copy in far_sends(slot, slot == 0) + near_sends(slot):
            copy.wait_send()
    if lead:
        pl.semaphore_wait(ready, len(beside))
        for copy in far_results(list(range(1, mp)) + [0]):
            copy.start()

    @pl.loop(lead, held)
    def _(slot):
        arrived(0, slot, chip * pair, pair)
        arrived(1, slot, 0, group)
        weigh(slot, 0)
        arrived(2, slot, 0, group)
        attend(slot + extra, slot, 0)
        for copy in far_sends(slot) + near_sends(slot):
            copy.wait_send()

        @pl.when(slot > lead)
        def _():
            settle(slot + extra - 1, slot - 1)

    for slot in range(lead):
        settle(slot + extra, slot)
    settle(held - 1 + extra, held - 1)
    for slot in range(lead):
        for step in range(1, others):
            settle(slot * (others - 1) + step - 1, slot, step)


def duo(
    heads, pieces,
    lengths, query, key, value, out,
    kept, weights, totals, results, table,
    landed, sent, result_in, result_out, table_in, ready,
):
    rows = query.shape[0]
    mp = lax.axis_size("mp")
    part = rows // mp
    wide = heads // 4
    slots = lengths.shape[1]
    seq_index = lax.axis_index("seq")
    mp_index = lax.axis_index("mp")
    bucket = seq_index // 4
    place = lax.rem(seq_index, 4)
    core = lax.rem(place, 2)
    chip = place // 2
    other = 1 - chip
    inputs = (query, key, value)

    def device(there_chip, there_core, there_mp):
        return {"seq": bucket * 4 + there_chip * 2 + there_core, "mp": there_mp}

    def lanes(piece, base=0):
        first, count = pieces[piece]
        return pl.ds(pl.multiple_of((base + first) * HD, HD), count * HD)

    def block_at(index):
        return pl.ds(pl.multiple_of(index * rows, rows), rows)

    def send(kind, piece, there_chip, there_core):
        return pltpu.make_async_remote_copy(
            src_ref=inputs[kind].at[:, lanes(piece, (there_core * 2 + there_chip) * wide)],
            dst_ref=kept.at[kind, block_at(place), lanes(piece)],
            send_sem=sent, recv_sem=landed.at[kind, piece],
            device_id=device(there_chip, there_core, mp_index), device_id_type=MESH,
        )

    def keep(kind, piece):
        return pltpu.make_async_copy(
            inputs[kind].at[:, lanes(piece, (core * 2 + chip) * wide)],
            kept.at[kind, block_at(place), lanes(piece)], landed.at[kind, piece],
        )

    def result(piece, there_chip, core_step, mp_step):
        there_core = core_step if there_chip is other else lax.rem(core + core_step, 2)
        there_mp = lax.rem(mp_index + mp_step, mp)
        first = (there_chip * 2 + there_core) * rows + there_mp * part
        source = results.at[pl.ds(pl.multiple_of(first, part), part), lanes(piece)]
        target = out.at[:, lanes(piece, mp_index * heads + (core * 2 + chip) * wide)]
        if there_chip is chip and core_step == 0 and mp_step == 0:
            target[...] = source[...]
            return
        pltpu.make_async_remote_copy(
            src_ref=source, dst_ref=target, send_sem=result_out, recv_sem=result_in,
            device_id=device(there_chip, there_core, there_mp), device_id_type=MESH,
        ).start()

    barrier = pltpu.get_barrier_semaphore()
    far = [device(other, b, mp_index) for b in range(2)]
    beside = [device(chip, b, lax.rem(mp_index + m, mp)) for m in range(1, mp) for b in range(2)]

    def greet(semaphore, devices):
        for there in devices:
            pl.semaphore_signal(semaphore, inc=1, device_id=there, device_id_type=MESH)

    greet(barrier, far)
    pl.when(chip == 0)(lambda: greet(barrier, beside))
    known = len(far) + lax.select(chip == 0, len(beside), 0)
    pl.semaphore_wait(barrier, known)

    for piece in range(len(pieces)):
        for kind in (1, 0, 2):
            for there_core in range(2):
                send(kind, piece, other, there_core).start()
    fetch = pltpu.make_async_copy(lengths, table, table_in)
    fetch.start()
    for piece in range(len(pieces)):
        for kind in (1, 0, 2):
            keep(kind, piece).start()

    greet(ready, far)

    @pl.when(chip == 0)
    def _():
        greet(ready, beside)
        pl.semaphore_wait(ready, len(far) + len(beside))
        greet(ready, far)

    pl.when(chip != 0)(lambda: pl.semaphore_wait(ready, 2 * len(far)))

    for piece in range(len(pieces)):
        for kind in (1, 0, 2):
            send(kind, piece, chip, 1 - core).start()

    fetch.wait()
    ends = []
    running = jnp.int32(0)
    for i in range(slots):
        running = running + table[bucket, i]
        ends.append(running)

    def ids(offset):
        found = jnp.zeros_like(offset)
        for end in ends:
            found = found + (offset >= end).astype(jnp.int32)
        return found

    k_ids = ids(lax.broadcasted_iota(jnp.int32, (1, 4 * rows), 1))
    factor = LOG2E / HD**0.5

    def arrived(kind, piece):
        ref = kept.at[kind, :, lanes(piece)]
        pltpu.make_async_copy(ref, ref, landed.at[kind, piece]).wait()

    def heads_of(piece):
        first, count = pieces[piece]
        return [(head, slice(head * HD, (head + 1) * HD)) for head in range(first, first + count)]

    def weigh(piece, index):
        block = block_at(index)
        q_ids = ids(lax.broadcasted_iota(jnp.int32, (rows, 1), 0) + index * rows)
        for head, lane in heads_of(piece):
            score = lax.dot_general(
                kept[0, block, lane], kept[1, :, lane],
                (((1,), (1,)), ((), ())), preferred_element_type=jnp.float32,
            )
            score = jnp.where(q_ids == k_ids, score, NEG)
            top = jnp.max(score, axis=1, keepdims=True)
            weight = jnp.exp2((score - top) * factor)
            totals[head, block, :] = jnp.broadcast_to(jnp.sum(weight, axis=1, keepdims=True), (rows, HD))
            weights[head, block, :] = weight.astype(jnp.bfloat16)

    def attend(piece, index):
        block = block_at(index)
        for head, lane in heads_of(piece):
            summed = jnp.dot(weights[head, block, :], kept[2, :, lane], preferred_element_type=jnp.float32)
            results[block, lane] = (summed / totals[head, block, :]).astype(jnp.bfloat16)

    def direct(piece):
        for core_step in range(2):
            result(piece, other, core_step, 0)

    def diagonal(piece):
        for mp_step in range(1, mp):
            for core_step in range(2):
                result(piece, other, core_step, mp_step)

    def own(piece):
        for core_step in reversed(range(2)):
            for mp_step in reversed(range(mp)):
                result(piece, chip, core_step, mp_step)

    def each(work, piece, there_chip):
        @pl.loop(0, 2)
        def _(step):
            work(piece, there_chip * 2 + step)

    last = len(pieces) - 1
    for piece in range(len(pieces)):
        arrived(1, piece)
        arrived(0, piece)
        each(weigh, piece, other)
        if piece < last:
            each(weigh, piece, chip)
        arrived(2, piece)
        if piece:
            diagonal(piece - 1)
        each(attend, piece, other)
        if piece == last:
            diagonal(piece)
        direct(piece)
        if piece == last:
            each(weigh, piece, chip)
        each(attend, piece, chip)
        own(piece)

    whole = kept.at[:, pl.ds(0, 3 * rows)]
    pltpu.make_async_copy(whole, whole, sent).wait()
    moved = out.at[:, pl.ds(0, out.shape[1] - wide * HD)]
    pltpu.make_async_copy(moved, moved, result_out).wait()
    pltpu.make_async_copy(moved, moved, result_in).wait()


def duo_call(query, key, value, clip_lengths):
    rows, width = query.shape
    heads = width // HD
    mp = lax.axis_size("mp")
    wide = heads // 4
    early = (wide + 1) // 2
    pieces = [(0, early)] + [(head, 1) for head in range(early, wide)]
    dma = pltpu.SemaphoreType.DMA
    whole = pl.BlockSpec(memory_space=pl.ANY)
    return pl.pallas_call(
        functools.partial(duo, heads, pieces),
        out_shape=pltpu.VMEM((rows // mp, width * mp), jnp.bfloat16),
        in_specs=[whole] * 4,
        out_specs=pl.BlockSpec(memory_space=pltpu.VMEM),
        scratch_shapes=[
            pltpu.VMEM((3, 4 * rows, wide * HD), jnp.bfloat16),
            pltpu.VMEM((wide, 4 * rows, 4 * rows), jnp.bfloat16),
            pltpu.VMEM((wide, 4 * rows, HD), jnp.float32),
            pltpu.VMEM((4 * rows, wide * HD), jnp.bfloat16),
            pltpu.SMEM(clip_lengths.shape, jnp.int32),
            dma((3, len(pieces))), dma(()), dma(()), dma(()), dma(()), pltpu.SemaphoreType.REGULAR,
        ],
        compiler_params=pltpu.CompilerParams(collective_id=0, has_side_effects=True),
        name="packed_attention",
    )(clip_lengths, query, key, value)


def shards(query, key, value, clip_lengths):
    rows, width = query.shape
    heads = width // HD
    group = lax.axis_size("seq") // clip_lengths.shape[0]
    mp = lax.axis_size("mp")
    if group == 4 and heads % 4 == 0 and rows % (16 * mp) == 0 and mp > 1:
        return duo_call(query, key, value, clip_lengths)
    pair = 2 if group % 2 == 0 and heads % 2 == 0 else 1
    per_core = heads // pair
    others = group // pair
    lead = min(2, (per_core - 1) // others) if others > 1 else 0
    held = per_core - lead * (others - 1)
    dma = pltpu.SemaphoreType.DMA
    whole = pl.BlockSpec(memory_space=pl.ANY)
    return pl.pallas_call(
        functools.partial(kernel, group, pair, mp, heads, lead),
        out_shape=pltpu.VMEM((rows // mp, width * mp), jnp.bfloat16),
        in_specs=[pl.BlockSpec(memory_space=pltpu.SMEM), whole, whole, whole],
        out_specs=pl.BlockSpec(memory_space=pltpu.VMEM),
        scratch_shapes=[
            pltpu.VMEM((held, group * rows, HD), jnp.bfloat16),
            pltpu.VMEM((held, group * rows, HD), jnp.bfloat16),
            pltpu.VMEM((held, group * rows, HD), jnp.bfloat16),
            pltpu.VMEM((per_core, pair * rows, HD), jnp.bfloat16),
            pltpu.VMEM((3, group, rows, HD), jnp.bfloat16),
            pltpu.VMEM((pair * rows, group * rows), jnp.bfloat16),
            pltpu.VMEM((pair * rows, HD), jnp.float32),
            dma((held, group)), dma((held, group)), dma((held, group)), dma((per_core, pair * mp)),
            dma((held, group)), dma((held, group)), dma((held, group)), dma((per_core, pair * mp)),
            dma((3, group)), pltpu.SemaphoreType.REGULAR,
        ],
        compiler_params=pltpu.CompilerParams(collective_id=0, has_side_effects=True),
        name="packed_attention",
    )(clip_lengths, query, key, value)


def solution(mesh):
    in_specs = (P("seq", "mp"), P("seq", "mp"), P("seq", "mp"), P())
    out_specs = P(("seq", "mp"), None)
    return jax.shard_map(shards, mesh=mesh, in_specs=in_specs, out_specs=out_specs, check_vma=False)
```

```python
import functools

import jax
import jax.numpy as jnp
from jax import lax
from jax.experimental import pallas as pl
from jax.experimental.pallas import tpu as pltpu
from jax.sharding import PartitionSpec as P

HD = 128
NEG = -1e30
LOG2E = 1.4426950408889634
MESH = pl.DeviceIdType.MESH


def kernel(
    group, pair, mp, heads, lead,
    lengths, query, key, value, out,
    q_buf, k_buf, v_buf, o_buf, first, p_buf, t_buf,
    q_in, k_in, v_in, o_in, q_out, k_out, v_out, o_out, first_in, ready,
):
    rows = query.shape[0]
    part = rows // mp
    per_core = heads // pair
    others = group // pair
    extra = lead * (others - 1)
    held = per_core - extra
    slots = lengths.shape[1]
    seq_index = lax.axis_index("seq")
    mp_index = lax.axis_index("mp")
    bucket = seq_index // group
    place = lax.rem(seq_index, group)
    core = lax.rem(place, pair)
    chip = place // pair

    def chip_at(chip_step):
        return lax.rem(chip + chip_step, others)

    def seq_of(chip_step, there_core):
        return bucket * group + chip_at(chip_step) * pair + there_core

    def head_of(slot, there_chip):
        if isinstance(slot, int) and slot < lead:
            return slot * others + there_chip
        return slot + extra

    def columns(owner, head):
        return pl.ds(pl.multiple_of((owner * per_core + head) * HD, HD), HD)

    def block_at(index):
        return pl.ds(pl.multiple_of(index * rows, rows), rows)

    kinds = ((query, q_buf, q_out, q_in), (key, k_buf, k_out, k_in), (value, v_buf, v_out, v_in))

    def local_copies(slot):
        mine = columns(core, head_of(slot, chip))
        return [
            pltpu.make_async_copy(source.at[:, mine], buf.at[slot, block_at(place), :], landed.at[slot, place])
            for source, buf, left, landed in kinds
        ]

    def far_kinds(slot):
        whole = isinstance(slot, int) and slot < lead
        return (0, 1, 2) if whole else (1, 2)

    far = [(chip_step, there_core) for there_core in range(pair) for chip_step in range(1, others)]

    def first_copies():
        return [
            pltpu.make_async_copy(
                kinds[kind][0].at[:, columns(there_core, head_of(0, chip_at(chip_step)))],
                first.at[kind, chip_step * pair + there_core],
                first_in.at[kind, chip_step * pair + there_core],
            )
            for kind in far_kinds(0) for chip_step, there_core in far
        ]

    def send(slot, chip_step, there_core, kind, staged=False):
        source, buf, left, landed = kinds[kind]
        index = chip_step * pair + there_core
        if staged:
            origin = first.at[kind, index]
        else:
            origin = source.at[:, columns(there_core, head_of(slot, chip_at(chip_step)))]
        return pltpu.make_async_remote_copy(
            src_ref=origin, dst_ref=buf.at[slot, block_at(place), :],
            send_sem=left.at[slot, index], recv_sem=landed.at[slot, place],
            device_id={"seq": seq_of(chip_step, there_core), "mp": mp_index}, device_id_type=MESH,
        )

    def far_sends(slot, staged=False):
        return [send(slot, a, b, kind, staged) for kind in far_kinds(slot) for a, b in far]

    def near_sends(slot):
        return [
            send(slot, 0, lax.rem(core + step, pair), kind)
            for kind in range(3) for step in range(1, pair)
        ]

    def result(turn, slot, chip_step, core_step, mp_step):
        there_core = lax.rem(core + core_step, pair)
        there_mp = lax.rem(mp_index + mp_step, mp)
        source = o_buf.at[turn, pl.ds(pl.multiple_of(there_core * rows + there_mp * part, part), part), :]
        column = (mp_index * heads + core * per_core + head_of(slot, chip)) * HD
        target = out.at[:, pl.ds(pl.multiple_of(column, HD), HD)]
        index = core_step * mp + mp_step
        if chip_step == 0 and index == 0:
            return pltpu.make_async_copy(source, target, o_in.at[turn, index])
        return pltpu.make_async_remote_copy(
            src_ref=source, dst_ref=target, send_sem=o_out.at[turn, index], recv_sem=o_in.at[turn, index],
            device_id={"seq": seq_of(chip_step, there_core), "mp": there_mp}, device_id_type=MESH,
        )

    for copy in first_copies():
        copy.start()

    barrier = pltpu.get_barrier_semaphore()
    beside = [(seq_of(0, b), lax.rem(mp_index + m, mp)) for b in range(pair) for m in range(1, mp)]
    greeted = [(seq_of(a, b), mp_index) for a, b in far]
    greeted += [(seq_of(0, lax.rem(core + b, pair)), mp_index) for b in range(1, pair)]
    greeted += beside
    for there_seq, there_mp in greeted:
        pl.semaphore_signal(
            barrier, inc=1, device_id={"seq": there_seq, "mp": there_mp}, device_id_type=MESH
        )

    for slot in range(max(lead, 1)):
        for copy in local_copies(slot):
            copy.start()

    @pl.loop(max(lead, 1), held)
    def _(slot):
        for copy in local_copies(slot):
            copy.start()

    ends = []
    running = jnp.int32(0)
    for i in range(slots):
        running = running + lengths[bucket, i]
        ends.append(running)

    def ids(offset):
        found = jnp.zeros_like(offset)
        for end in ends:
            found = found + (offset >= end).astype(jnp.int32)
        return found

    k_ids = ids(lax.broadcasted_iota(jnp.int32, (1, group * rows), 1))

    for copy in first_copies():
        copy.wait()
    pl.semaphore_wait(barrier, len(greeted))

    for slot in range(max(lead, 1)):
        for copy in far_sends(slot, slot == 0) + near_sends(slot):
            copy.start()

    @pl.loop(max(lead, 1), held)
    def _(slot):
        for copy in far_sends(slot) + near_sends(slot):
            copy.start()

    if lead:
        for there_seq, there_mp in beside:
            pl.semaphore_signal(
                ready, inc=1, device_id={"seq": there_seq, "mp": there_mp}, device_id_type=MESH
            )

    def arrived(kind, slot, base, count):
        buf, landed = kinds[kind][1], kinds[kind][3]
        for i in range(count):
            ref = buf.at[slot, block_at(base + i), :]
            pltpu.make_async_copy(ref, ref, landed.at[slot, base + i]).wait()

    factor = LOG2E / HD**0.5

    def weigh(slot, chip_step):
        keys = k_buf[slot]
        for b in range(pair):
            block = pl.ds(b * rows, rows)
            from_row = (chip_at(chip_step) * pair + b) * rows
            q_ids = ids(lax.broadcasted_iota(jnp.int32, (rows, 1), 0) + from_row)
            score = lax.dot_general(
                q_buf[slot, pl.ds(pl.multiple_of(from_row, rows), rows), :], keys,
                (((1,), (1,)), ((), ())), preferred_element_type=jnp.float32,
            )
            score = jnp.where(q_ids == k_ids, score, NEG)
            top = jnp.max(score, axis=1, keepdims=True)
            weight = jnp.exp2((score - top) * factor)
            t_buf[block, :] = jnp.broadcast_to(jnp.sum(weight, axis=1, keepdims=True), (rows, HD))
            p_buf[block, :] = weight.astype(jnp.bfloat16)

    def attend(turn, slot, chip_step):
        for core_step in reversed(range(pair)):
            block = block_at(lax.rem(core + core_step, pair))
            summed = jnp.dot(p_buf[block, :], v_buf[slot], preferred_element_type=jnp.float32)
            o_buf[turn, block, :] = (summed / t_buf[block, :]).astype(jnp.bfloat16)
            if chip_step == 0:
                for mp_step in reversed(range(mp)):
                    result(turn, slot, 0, core_step, mp_step).start()

    def far_results(mp_steps):
        return [
            result(slot * (others - 1) + a - 1, slot, a, core_step, mp_step)
            for slot in range(lead) for mp_step in mp_steps
            for core_step in range(pair) for a in range(1, others)
        ]

    def settle(turn, slot, chip_step=0):
        for core_step in range(pair):
            for mp_step in range(mp):
                copy = result(turn, slot, chip_step, core_step, mp_step)
                if chip_step == 0 and core_step == 0 and mp_step == 0:
                    copy.wait()
                else:
                    copy.wait_send()
                    copy.wait_recv()

    for slot in range(lead):
        arrived(0, slot, 0, group)
        arrived(1, slot, 0, group)
        for step in range(1, others):
            weigh(slot, step)
            if step == 1:
                arrived(2, slot, 0, group)
            attend(slot * (others - 1) + step - 1, slot, step)
        weigh(slot, 0)
        attend(slot + extra, slot, 0)
        for copy in far_sends(slot, slot == 0) + near_sends(slot):
            copy.wait_send()
    if lead:
        pl.semaphore_wait(ready, len(beside))
        for copy in far_results(list(range(1, mp)) + [0]):
            copy.start()

    @pl.loop(lead, held)
    def _(slot):
        arrived(0, slot, chip * pair, pair)
        arrived(1, slot, 0, group)
        weigh(slot, 0)
        arrived(2, slot, 0, group)
        attend(slot + extra, slot, 0)
        for copy in far_sends(slot) + near_sends(slot):
            copy.wait_send()

        @pl.when(slot > lead)
        def _():
            settle(slot + extra - 1, slot - 1)

    for slot in range(lead):
        settle(slot + extra, slot)
    settle(held - 1 + extra, held - 1)
    for slot in range(lead):
        for step in range(1, others):
            settle(slot * (others - 1) + step - 1, slot, step)


def duo(
    heads, pieces,
    lengths, query, key, value, out,
    kept, weights, totals, results, table,
    landed, sent, result_in, result_out, table_in, ready,
):
    rows = query.shape[0]
    mp = lax.axis_size("mp")
    part = rows // mp
    wide = heads // 4
    slots = lengths.shape[1]
    seq_index = lax.axis_index("seq")
    mp_index = lax.axis_index("mp")
    bucket = seq_index // 4
    place = lax.rem(seq_index, 4)
    core = lax.rem(place, 2)
    chip = place // 2
    other = 1 - chip
    inputs = (query, key, value)

    def device(there_chip, there_core, there_mp):
        return {"seq": bucket * 4 + there_chip * 2 + there_core, "mp": there_mp}

    def lanes(piece, base=0):
        first, count = pieces[piece]
        return pl.ds(pl.multiple_of((base + first) * HD, HD), count * HD)

    def block_at(index):
        return pl.ds(pl.multiple_of(index * rows, rows), rows)

    def send(kind, piece, there_chip, there_core):
        return pltpu.make_async_remote_copy(
            src_ref=inputs[kind].at[:, lanes(piece, (there_core * 2 + there_chip) * wide)],
            dst_ref=kept.at[kind, block_at(place), lanes(piece)],
            send_sem=sent, recv_sem=landed.at[kind, piece],
            device_id=device(there_chip, there_core, mp_index), device_id_type=MESH,
        )

    def keep(kind, piece):
        return pltpu.make_async_copy(
            inputs[kind].at[:, lanes(piece, (core * 2 + chip) * wide)],
            kept.at[kind, block_at(place), lanes(piece)], landed.at[kind, piece],
        )

    def result(piece, there_chip, core_step, mp_step):
        there_core = core_step if there_chip is other else lax.rem(core + core_step, 2)
        there_mp = lax.rem(mp_index + mp_step, mp)
        first = (there_chip * 2 + there_core) * rows + there_mp * part
        source = results.at[pl.ds(pl.multiple_of(first, part), part), lanes(piece)]
        target = out.at[:, lanes(piece, mp_index * heads + (core * 2 + chip) * wide)]
        if there_chip is chip and core_step == 0 and mp_step == 0:
            target[...] = source[...]
            return
        pltpu.make_async_remote_copy(
            src_ref=source, dst_ref=target, send_sem=result_out, recv_sem=result_in,
            device_id=device(there_chip, there_core, there_mp), device_id_type=MESH,
        ).start()

    barrier = pltpu.get_barrier_semaphore()
    far = [device(other, b, mp_index) for b in range(2)]
    beside = [device(chip, b, lax.rem(mp_index + m, mp)) for m in range(1, mp) for b in range(2)]

    def greet(semaphore, devices):
        for there in devices:
            pl.semaphore_signal(semaphore, inc=1, device_id=there, device_id_type=MESH)

    greet(barrier, far)
    pl.when(chip == 0)(lambda: greet(barrier, beside))
    known = len(far) + lax.select(chip == 0, len(beside), 0)
    pl.semaphore_wait(barrier, known)

    for piece in range(len(pieces)):
        for kind in (1, 0, 2):
            for there_core in range(2):
                send(kind, piece, other, there_core).start()
    fetch = pltpu.make_async_copy(lengths, table, table_in)
    fetch.start()
    for piece in range(len(pieces)):
        for kind in (1, 0, 2):
            keep(kind, piece).start()

    greet(ready, far)

    @pl.when(chip == 0)
    def _():
        greet(ready, beside)
        pl.semaphore_wait(ready, len(far) + len(beside))
        greet(ready, far)

    pl.when(chip != 0)(lambda: pl.semaphore_wait(ready, 2 * len(far)))

    for piece in range(len(pieces)):
        for kind in (1, 0, 2):
            send(kind, piece, chip, 1 - core).start()

    fetch.wait()
    ends = []
    running = jnp.int32(0)
    for i in range(slots):
        running = running + table[bucket, i]
        ends.append(running)

    def ids(offset):
        found = jnp.zeros_like(offset)
        for end in ends:
            found = found + (offset >= end).astype(jnp.int32)
        return found

    k_ids = ids(lax.broadcasted_iota(jnp.int32, (1, 4 * rows), 1))
    factor = LOG2E / HD**0.5

    def arrived(kind, piece):
        ref = kept.at[kind, :, lanes(piece)]
        pltpu.make_async_copy(ref, ref, landed.at[kind, piece]).wait()

    def heads_of(piece):
        first, count = pieces[piece]
        return [(head, slice(head * HD, (head + 1) * HD)) for head in range(first, first + count)]

    def weigh(piece, index):
        block = block_at(index)
        q_ids = ids(lax.broadcasted_iota(jnp.int32, (rows, 1), 0) + index * rows)
        for head, lane in heads_of(piece):
            score = lax.dot_general(
                kept[0, block, lane], kept[1, :, lane],
                (((1,), (1,)), ((), ())), preferred_element_type=jnp.float32,
            )
            score = jnp.where(q_ids == k_ids, score, NEG)
            top = jnp.max(score, axis=1, keepdims=True)
            weight = jnp.exp2((score - top) * factor)
            totals[head, block, :] = jnp.broadcast_to(jnp.sum(weight, axis=1, keepdims=True), (rows, HD))
            weights[head, block, :] = weight.astype(jnp.bfloat16)

    def attend(piece, index, count=1):
        block = pl.ds(pl.multiple_of(index * count * rows, count * rows), count * rows)
        for head, lane in heads_of(piece):
            summed = jnp.dot(weights[head, block, :], kept[2, :, lane], preferred_element_type=jnp.float32)
            results[block, lane] = (summed / totals[head, block, :]).astype(jnp.bfloat16)

    def direct(piece):
        for core_step in range(2):
            result(piece, other, core_step, 0)

    def diagonal(piece):
        for mp_step in range(1, mp):
            for core_step in range(2):
                result(piece, other, core_step, mp_step)

    def own(piece):
        for core_step in reversed(range(2)):
            for mp_step in reversed(range(mp)):
                result(piece, chip, core_step, mp_step)

    def each(work, piece, there_chip):
        @pl.loop(0, 2)
        def _(step):
            work(piece, there_chip * 2 + step)

    last = len(pieces) - 1
    for piece in range(len(pieces)):
        arrived(1, piece)
        arrived(0, piece)
        each(weigh, piece, other)
        if piece < last:
            each(weigh, piece, chip)
        arrived(2, piece)
        if piece:
            diagonal(piece - 1)
        if piece == last:
            attend(piece, other, 2)
        else:
            each(attend, piece, other)
        if piece == last:
            diagonal(piece)
        direct(piece)
        if piece == last:
            each(weigh, piece, chip)
        each(attend, piece, chip)
        own(piece)

    whole = kept.at[:, pl.ds(0, 3 * rows)]
    pltpu.make_async_copy(whole, whole, sent).wait()
    moved = out.at[:, pl.ds(0, out.shape[1] - wide * HD)]
    pltpu.make_async_copy(moved, moved, result_out).wait()
    pltpu.make_async_copy(moved, moved, result_in).wait()


def duo_call(query, key, value, clip_lengths):
    rows, width = query.shape
    heads = width // HD
    mp = lax.axis_size("mp")
    wide = heads // 4
    early = (wide + 1) // 2
    pieces = [(0, early)] + [(head, 1) for head in range(early, wide)]
    dma = pltpu.SemaphoreType.DMA
    whole = pl.BlockSpec(memory_space=pl.ANY)
    return pl.pallas_call(
        functools.partial(duo, heads, pieces),
        out_shape=pltpu.VMEM((rows // mp, width * mp), jnp.bfloat16),
        in_specs=[whole] * 4,
        out_specs=pl.BlockSpec(memory_space=pltpu.VMEM),
        scratch_shapes=[
            pltpu.VMEM((3, 4 * rows, wide * HD), jnp.bfloat16),
            pltpu.VMEM((wide, 4 * rows, 4 * rows), jnp.bfloat16),
            pltpu.VMEM((wide, 4 * rows, HD), jnp.float32),
            pltpu.VMEM((4 * rows, wide * HD), jnp.bfloat16),
            pltpu.SMEM(clip_lengths.shape, jnp.int32),
            dma((3, len(pieces))), dma(()), dma(()), dma(()), dma(()), pltpu.SemaphoreType.REGULAR,
        ],
        compiler_params=pltpu.CompilerParams(collective_id=0, has_side_effects=True),
        name="packed_attention",
    )(clip_lengths, query, key, value)


def shards(query, key, value, clip_lengths):
    rows, width = query.shape
    heads = width // HD
    group = lax.axis_size("seq") // clip_lengths.shape[0]
    mp = lax.axis_size("mp")
    if group == 4 and heads % 4 == 0 and rows % (16 * mp) == 0 and mp > 1:
        return duo_call(query, key, value, clip_lengths)
    pair = 2 if group % 2 == 0 and heads % 2 == 0 else 1
    per_core = heads // pair
    others = group // pair
    lead = min(2, (per_core - 1) // others) if others > 1 else 0
    held = per_core - lead * (others - 1)
    dma = pltpu.SemaphoreType.DMA
    whole = pl.BlockSpec(memory_space=pl.ANY)
    return pl.pallas_call(
        functools.partial(kernel, group, pair, mp, heads, lead),
        out_shape=pltpu.VMEM((rows // mp, width * mp), jnp.bfloat16),
        in_specs=[pl.BlockSpec(memory_space=pltpu.SMEM), whole, whole, whole],
        out_specs=pl.BlockSpec(memory_space=pltpu.VMEM),
        scratch_shapes=[
            pltpu.VMEM((held, group * rows, HD), jnp.bfloat16),
            pltpu.VMEM((held, group * rows, HD), jnp.bfloat16),
            pltpu.VMEM((held, group * rows, HD), jnp.bfloat16),
            pltpu.VMEM((per_core, pair * rows, HD), jnp.bfloat16),
            pltpu.VMEM((3, group, rows, HD), jnp.bfloat16),
            pltpu.VMEM((pair * rows, group * rows), jnp.bfloat16),
            pltpu.VMEM((pair * rows, HD), jnp.float32),
            dma((held, group)), dma((held, group)), dma((held, group)), dma((per_core, pair * mp)),
            dma((held, group)), dma((held, group)), dma((held, group)), dma((per_core, pair * mp)),
            dma((3, group)), pltpu.SemaphoreType.REGULAR,
        ],
        compiler_params=pltpu.CompilerParams(collective_id=0, has_side_effects=True),
        name="packed_attention",
    )(clip_lengths, query, key, value)


def solution(mesh):
    in_specs = (P("seq", "mp"), P("seq", "mp"), P("seq", "mp"), P())
    out_specs = P(("seq", "mp"), None)
    return jax.shard_map(shards, mesh=mesh, in_specs=in_specs, out_specs=out_specs, check_vma=False)
```

```python
import functools

import jax
import jax.numpy as jnp
from jax import lax
from jax.experimental import pallas as pl
from jax.experimental.pallas import tpu as pltpu
from jax.sharding import PartitionSpec as P

HD = 128
NEG = -1e30
LOG2E = 1.4426950408889634
MESH = pl.DeviceIdType.MESH


def kernel(
    group, pair, mp, heads, lead,
    lengths, query, key, value, out,
    q_buf, k_buf, v_buf, o_buf, first, p_buf, t_buf,
    q_in, k_in, v_in, o_in, q_out, k_out, v_out, o_out, first_in, ready,
):
    rows = query.shape[0]
    part = rows // mp
    per_core = heads // pair
    others = group // pair
    extra = lead * (others - 1)
    held = per_core - extra
    slots = lengths.shape[1]
    seq_index = lax.axis_index("seq")
    mp_index = lax.axis_index("mp")
    bucket = seq_index // group
    place = lax.rem(seq_index, group)
    core = lax.rem(place, pair)
    chip = place // pair

    def chip_at(chip_step):
        return lax.rem(chip + chip_step, others)

    def seq_of(chip_step, there_core):
        return bucket * group + chip_at(chip_step) * pair + there_core

    def head_of(slot, there_chip):
        if isinstance(slot, int) and slot < lead:
            return slot * others + there_chip
        return slot + extra

    def columns(owner, head):
        return pl.ds(pl.multiple_of((owner * per_core + head) * HD, HD), HD)

    def block_at(index):
        return pl.ds(pl.multiple_of(index * rows, rows), rows)

    kinds = ((query, q_buf, q_out, q_in), (key, k_buf, k_out, k_in), (value, v_buf, v_out, v_in))

    def local_copies(slot):
        mine = columns(core, head_of(slot, chip))
        return [
            pltpu.make_async_copy(source.at[:, mine], buf.at[slot, block_at(place), :], landed.at[slot, place])
            for source, buf, left, landed in kinds
        ]

    def far_kinds(slot):
        whole = isinstance(slot, int) and slot < lead
        return (0, 1, 2) if whole else (1, 2)

    far = [(chip_step, there_core) for there_core in range(pair) for chip_step in range(1, others)]

    def first_copies():
        return [
            pltpu.make_async_copy(
                kinds[kind][0].at[:, columns(there_core, head_of(0, chip_at(chip_step)))],
                first.at[kind, chip_step * pair + there_core],
                first_in.at[kind, chip_step * pair + there_core],
            )
            for kind in far_kinds(0) for chip_step, there_core in far
        ]

    def send(slot, chip_step, there_core, kind, staged=False):
        source, buf, left, landed = kinds[kind]
        index = chip_step * pair + there_core
        if staged:
            origin = first.at[kind, index]
        else:
            origin = source.at[:, columns(there_core, head_of(slot, chip_at(chip_step)))]
        return pltpu.make_async_remote_copy(
            src_ref=origin, dst_ref=buf.at[slot, block_at(place), :],
            send_sem=left.at[slot, index], recv_sem=landed.at[slot, place],
            device_id={"seq": seq_of(chip_step, there_core), "mp": mp_index}, device_id_type=MESH,
        )

    def far_sends(slot, staged=False):
        return [send(slot, a, b, kind, staged) for kind in far_kinds(slot) for a, b in far]

    def near_sends(slot):
        return [
            send(slot, 0, lax.rem(core + step, pair), kind)
            for kind in range(3) for step in range(1, pair)
        ]

    def result(turn, slot, chip_step, core_step, mp_step):
        there_core = lax.rem(core + core_step, pair)
        there_mp = lax.rem(mp_index + mp_step, mp)
        source = o_buf.at[turn, pl.ds(pl.multiple_of(there_core * rows + there_mp * part, part), part), :]
        column = (mp_index * heads + core * per_core + head_of(slot, chip)) * HD
        target = out.at[:, pl.ds(pl.multiple_of(column, HD), HD)]
        index = core_step * mp + mp_step
        if chip_step == 0 and index == 0:
            return pltpu.make_async_copy(source, target, o_in.at[turn, index])
        return pltpu.make_async_remote_copy(
            src_ref=source, dst_ref=target, send_sem=o_out.at[turn, index], recv_sem=o_in.at[turn, index],
            device_id={"seq": seq_of(chip_step, there_core), "mp": there_mp}, device_id_type=MESH,
        )

    for copy in first_copies():
        copy.start()

    barrier = pltpu.get_barrier_semaphore()
    beside = [(seq_of(0, b), lax.rem(mp_index + m, mp)) for b in range(pair) for m in range(1, mp)]
    greeted = [(seq_of(a, b), mp_index) for a, b in far]
    greeted += [(seq_of(0, lax.rem(core + b, pair)), mp_index) for b in range(1, pair)]
    greeted += beside
    for there_seq, there_mp in greeted:
        pl.semaphore_signal(
            barrier, inc=1, device_id={"seq": there_seq, "mp": there_mp}, device_id_type=MESH
        )

    for slot in range(max(lead, 1)):
        for copy in local_copies(slot):
            copy.start()

    @pl.loop(max(lead, 1), held)
    def _(slot):
        for copy in local_copies(slot):
            copy.start()

    ends = []
    running = jnp.int32(0)
    for i in range(slots):
        running = running + lengths[bucket, i]
        ends.append(running)

    def ids(offset):
        found = jnp.zeros_like(offset)
        for end in ends:
            found = found + (offset >= end).astype(jnp.int32)
        return found

    k_ids = ids(lax.broadcasted_iota(jnp.int32, (1, group * rows), 1))

    for copy in first_copies():
        copy.wait()
    pl.semaphore_wait(barrier, len(greeted))

    for slot in range(max(lead, 1)):
        for copy in far_sends(slot, slot == 0) + near_sends(slot):
            copy.start()

    @pl.loop(max(lead, 1), held)
    def _(slot):
        for copy in far_sends(slot) + near_sends(slot):
            copy.start()

    if lead:
        for there_seq, there_mp in beside:
            pl.semaphore_signal(
                ready, inc=1, device_id={"seq": there_seq, "mp": there_mp}, device_id_type=MESH
            )

    def arrived(kind, slot, base, count):
        buf, landed = kinds[kind][1], kinds[kind][3]
        for i in range(count):
            ref = buf.at[slot, block_at(base + i), :]
            pltpu.make_async_copy(ref, ref, landed.at[slot, base + i]).wait()

    factor = LOG2E / HD**0.5

    def weigh(slot, chip_step):
        keys = k_buf[slot]
        for b in range(pair):
            block = pl.ds(b * rows, rows)
            from_row = (chip_at(chip_step) * pair + b) * rows
            q_ids = ids(lax.broadcasted_iota(jnp.int32, (rows, 1), 0) + from_row)
            score = lax.dot_general(
                q_buf[slot, pl.ds(pl.multiple_of(from_row, rows), rows), :], keys,
                (((1,), (1,)), ((), ())), preferred_element_type=jnp.float32,
            )
            score = jnp.where(q_ids == k_ids, score, NEG)
            top = jnp.max(score, axis=1, keepdims=True)
            weight = jnp.exp2((score - top) * factor)
            t_buf[block, :] = jnp.broadcast_to(jnp.sum(weight, axis=1, keepdims=True), (rows, HD))
            p_buf[block, :] = weight.astype(jnp.bfloat16)

    def attend(turn, slot, chip_step):
        for core_step in reversed(range(pair)):
            block = block_at(lax.rem(core + core_step, pair))
            summed = jnp.dot(p_buf[block, :], v_buf[slot], preferred_element_type=jnp.float32)
            o_buf[turn, block, :] = (summed / t_buf[block, :]).astype(jnp.bfloat16)
            if chip_step == 0:
                for mp_step in reversed(range(mp)):
                    result(turn, slot, 0, core_step, mp_step).start()

    def far_results(mp_steps):
        return [
            result(slot * (others - 1) + a - 1, slot, a, core_step, mp_step)
            for slot in range(lead) for mp_step in mp_steps
            for core_step in range(pair) for a in range(1, others)
        ]

    def settle(turn, slot, chip_step=0):
        for core_step in range(pair):
            for mp_step in range(mp):
                copy = result(turn, slot, chip_step, core_step, mp_step)
                if chip_step == 0 and core_step == 0 and mp_step == 0:
                    copy.wait()
                else:
                    copy.wait_send()
                    copy.wait_recv()

    for slot in range(lead):
        arrived(0, slot, 0, group)
        arrived(1, slot, 0, group)
        for step in range(1, others):
            weigh(slot, step)
            if step == 1:
                arrived(2, slot, 0, group)
            attend(slot * (others - 1) + step - 1, slot, step)
        weigh(slot, 0)
        attend(slot + extra, slot, 0)
        for copy in far_sends(slot, slot == 0) + near_sends(slot):
            copy.wait_send()
    if lead:
        pl.semaphore_wait(ready, len(beside))
        for copy in far_results(list(range(1, mp)) + [0]):
            copy.start()

    @pl.loop(lead, held)
    def _(slot):
        arrived(0, slot, chip * pair, pair)
        arrived(1, slot, 0, group)
        weigh(slot, 0)
        arrived(2, slot, 0, group)
        attend(slot + extra, slot, 0)
        for copy in far_sends(slot) + near_sends(slot):
            copy.wait_send()

        @pl.when(slot > lead)
        def _():
            settle(slot + extra - 1, slot - 1)

    for slot in range(lead):
        settle(slot + extra, slot)
    settle(held - 1 + extra, held - 1)
    for slot in range(lead):
        for step in range(1, others):
            settle(slot * (others - 1) + step - 1, slot, step)


def duo(
    heads, pieces,
    lengths, query, key, value, out,
    kept, weights, totals, results, table,
    landed, sent, result_in, result_out, table_in, ready,
):
    rows = query.shape[0]
    mp = lax.axis_size("mp")
    part = rows // mp
    wide = heads // 4
    slots = lengths.shape[1]
    seq_index = lax.axis_index("seq")
    mp_index = lax.axis_index("mp")
    bucket = seq_index // 4
    place = lax.rem(seq_index, 4)
    core = lax.rem(place, 2)
    chip = place // 2
    other = 1 - chip
    inputs = (query, key, value)

    def device(there_chip, there_core, there_mp):
        return {"seq": bucket * 4 + there_chip * 2 + there_core, "mp": there_mp}

    def lanes(piece, base=0):
        first, count = pieces[piece]
        return pl.ds(pl.multiple_of((base + first) * HD, HD), count * HD)

    def block_at(index):
        return pl.ds(pl.multiple_of(index * rows, rows), rows)

    def send(kind, piece, there_chip, there_core):
        return pltpu.make_async_remote_copy(
            src_ref=inputs[kind].at[:, lanes(piece, (there_core * 2 + there_chip) * wide)],
            dst_ref=kept.at[kind, block_at(place), lanes(piece)],
            send_sem=sent, recv_sem=landed.at[kind, piece],
            device_id=device(there_chip, there_core, mp_index), device_id_type=MESH,
        )

    def keep(kind, piece):
        return pltpu.make_async_copy(
            inputs[kind].at[:, lanes(piece, (core * 2 + chip) * wide)],
            kept.at[kind, block_at(place), lanes(piece)], landed.at[kind, piece],
        )

    def result(piece, there_chip, core_step, mp_step):
        there_core = core_step if there_chip is other else lax.rem(core + core_step, 2)
        there_mp = lax.rem(mp_index + mp_step, mp)
        first = (there_chip * 2 + there_core) * rows + there_mp * part
        source = results.at[pl.ds(pl.multiple_of(first, part), part), lanes(piece)]
        target = out.at[:, lanes(piece, mp_index * heads + (core * 2 + chip) * wide)]
        if there_chip is chip and core_step == 0 and mp_step == 0:
            target[...] = source[...]
            return
        pltpu.make_async_remote_copy(
            src_ref=source, dst_ref=target, send_sem=result_out, recv_sem=result_in,
            device_id=device(there_chip, there_core, there_mp), device_id_type=MESH,
        ).start()

    barrier = pltpu.get_barrier_semaphore()
    far = [device(other, b, mp_index) for b in range(2)]
    beside = [device(chip, b, lax.rem(mp_index + m, mp)) for m in range(1, mp) for b in range(2)]

    def greet(semaphore, devices):
        for there in devices:
            pl.semaphore_signal(semaphore, inc=1, device_id=there, device_id_type=MESH)

    greet(barrier, far)
    pl.when(chip == 0)(lambda: greet(barrier, beside))
    known = len(far) + lax.select(chip == 0, len(beside), 0)
    pl.semaphore_wait(barrier, known)

    for piece in range(len(pieces)):
        for kind in (1, 0, 2):
            for there_core in range(2):
                send(kind, piece, other, there_core).start()
    fetch = pltpu.make_async_copy(lengths, table, table_in)
    fetch.start()
    for piece in range(len(pieces)):
        for kind in (1, 0, 2):
            keep(kind, piece).start()

    greet(ready, far)

    @pl.when(chip == 0)
    def _():
        greet(ready, beside)
        pl.semaphore_wait(ready, len(far) + len(beside))
        greet(ready, far)

    pl.when(chip != 0)(lambda: pl.semaphore_wait(ready, 2 * len(far)))

    for piece in range(len(pieces)):
        for kind in (1, 0, 2):
            send(kind, piece, chip, 1 - core).start()

    fetch.wait()
    ends = []
    running = jnp.int32(0)
    for i in range(slots):
        running = running + table[bucket, i]
        ends.append(running)

    def ids(offset):
        found = jnp.zeros_like(offset)
        for end in ends:
            found = found + (offset >= end).astype(jnp.int32)
        return found

    k_ids = ids(lax.broadcasted_iota(jnp.int32, (1, 4 * rows), 1))
    factor = LOG2E / HD**0.5

    def arrived(kind, piece):
        ref = kept.at[kind, :, lanes(piece)]
        pltpu.make_async_copy(ref, ref, landed.at[kind, piece]).wait()

    def heads_of(piece):
        first, count = pieces[piece]
        return [(head, slice(head * HD, (head + 1) * HD)) for head in range(first, first + count)]

    def weigh(piece, index):
        block = block_at(index)
        q_ids = ids(lax.broadcasted_iota(jnp.int32, (rows, 1), 0) + index * rows)
        for head, lane in heads_of(piece):
            score = lax.dot_general(
                kept[0, block, lane], kept[1, :, lane],
                (((1,), (1,)), ((), ())), preferred_element_type=jnp.float32,
            )
            score = jnp.where(q_ids == k_ids, score, NEG)
            top = jnp.max(score, axis=1, keepdims=True)
            weight = jnp.exp2((score - top) * factor)
            totals[head, block, :] = jnp.broadcast_to(jnp.sum(weight, axis=1, keepdims=True), (rows, HD))
            weights[head, block, :] = weight.astype(jnp.bfloat16)

    def attend(piece, index, count=1):
        block = pl.ds(pl.multiple_of(index * count * rows, count * rows), count * rows)
        for head, lane in heads_of(piece):
            summed = jnp.dot(weights[head, block, :], kept[2, :, lane], preferred_element_type=jnp.float32)
            results[block, lane] = (summed / totals[head, block, :]).astype(jnp.bfloat16)

    def direct(piece):
        for core_step in range(2):
            result(piece, other, core_step, 0)

    def diagonal(piece, cores=(0, 1)):
        for mp_step in range(1, mp):
            for core_step in cores:
                result(piece, other, core_step, mp_step)

    def own(piece):
        for core_step in reversed(range(2)):
            for mp_step in reversed(range(mp)):
                result(piece, chip, core_step, mp_step)

    def each(work, piece, there_chip):
        @pl.loop(0, 2)
        def _(step):
            work(piece, there_chip * 2 + step)

    last = len(pieces) - 1
    for piece in range(len(pieces)):
        arrived(1, piece)
        arrived(0, piece)
        each(weigh, piece, other)
        if piece < last:
            each(weigh, piece, chip)
        if piece:
            both = jnp.logical_and(mp_index == 1, chip == 1)
            pl.when(mp_index == 1)(lambda: diagonal(piece - 1, (0,)))
            pl.when(both)(lambda: diagonal(piece - 1, (1,)))
        arrived(2, piece)
        if piece:
            pl.when(mp_index != 1)(lambda: diagonal(piece - 1, (0,)))
            pl.when(jnp.logical_not(both))(lambda: diagonal(piece - 1, (1,)))
        if piece == last:
            attend(piece, other, 2)
        else:
            each(attend, piece, other)
        if piece == last:
            diagonal(piece)
        direct(piece)
        if piece == last:
            each(weigh, piece, chip)
        each(attend, piece, chip)
        own(piece)

    whole = kept.at[:, pl.ds(0, 3 * rows)]
    pltpu.make_async_copy(whole, whole, sent).wait()
    moved = out.at[:, pl.ds(0, out.shape[1] - wide * HD)]
    pltpu.make_async_copy(moved, moved, result_out).wait()
    pltpu.make_async_copy(moved, moved, result_in).wait()


def duo_call(query, key, value, clip_lengths):
    rows, width = query.shape
    heads = width // HD
    mp = lax.axis_size("mp")
    wide = heads // 4
    early = (wide + 1) // 2
    pieces = [(0, early)] + [(head, 1) for head in range(early, wide)]
    dma = pltpu.SemaphoreType.DMA
    whole = pl.BlockSpec(memory_space=pl.ANY)
    return pl.pallas_call(
        functools.partial(duo, heads, pieces),
        out_shape=pltpu.VMEM((rows // mp, width * mp), jnp.bfloat16),
        in_specs=[whole] * 4,
        out_specs=pl.BlockSpec(memory_space=pltpu.VMEM),
        scratch_shapes=[
            pltpu.VMEM((3, 4 * rows, wide * HD), jnp.bfloat16),
            pltpu.VMEM((wide, 4 * rows, 4 * rows), jnp.bfloat16),
            pltpu.VMEM((wide, 4 * rows, HD), jnp.float32),
            pltpu.VMEM((4 * rows, wide * HD), jnp.bfloat16),
            pltpu.SMEM(clip_lengths.shape, jnp.int32),
            dma((3, len(pieces))), dma(()), dma(()), dma(()), dma(()), pltpu.SemaphoreType.REGULAR,
        ],
        compiler_params=pltpu.CompilerParams(collective_id=0, has_side_effects=True),
        name="packed_attention",
    )(clip_lengths, query, key, value)


def shards(query, key, value, clip_lengths):
    rows, width = query.shape
    heads = width // HD
    group = lax.axis_size("seq") // clip_lengths.shape[0]
    mp = lax.axis_size("mp")
    if group == 4 and heads % 4 == 0 and rows % (16 * mp) == 0 and mp > 1:
        return duo_call(query, key, value, clip_lengths)
    pair = 2 if group % 2 == 0 and heads % 2 == 0 else 1
    per_core = heads // pair
    others = group // pair
    lead = min(2, (per_core - 1) // others) if others > 1 else 0
    held = per_core - lead * (others - 1)
    dma = pltpu.SemaphoreType.DMA
    whole = pl.BlockSpec(memory_space=pl.ANY)
    return pl.pallas_call(
        functools.partial(kernel, group, pair, mp, heads, lead),
        out_shape=pltpu.VMEM((rows // mp, width * mp), jnp.bfloat16),
        in_specs=[pl.BlockSpec(memory_space=pltpu.SMEM), whole, whole, whole],
        out_specs=pl.BlockSpec(memory_space=pltpu.VMEM),
        scratch_shapes=[
            pltpu.VMEM((held, group * rows, HD), jnp.bfloat16),
            pltpu.VMEM((held, group * rows, HD), jnp.bfloat16),
            pltpu.VMEM((held, group * rows, HD), jnp.bfloat16),
            pltpu.VMEM((per_core, pair * rows, HD), jnp.bfloat16),
            pltpu.VMEM((3, group, rows, HD), jnp.bfloat16),
            pltpu.VMEM((pair * rows, group * rows), jnp.bfloat16),
            pltpu.VMEM((pair * rows, HD), jnp.float32),
            dma((held, group)), dma((held, group)), dma((held, group)), dma((per_core, pair * mp)),
            dma((held, group)), dma((held, group)), dma((held, group)), dma((per_core, pair * mp)),
            dma((3, group)), pltpu.SemaphoreType.REGULAR,
        ],
        compiler_params=pltpu.CompilerParams(collective_id=0, has_side_effects=True),
        name="packed_attention",
    )(clip_lengths, query, key, value)


def solution(mesh):
    in_specs = (P("seq", "mp"), P("seq", "mp"), P("seq", "mp"), P())
    out_specs = P(("seq", "mp"), None)
    return jax.shard_map(shards, mesh=mesh, in_specs=in_specs, out_specs=out_specs, check_vma=False)
```

```python
import functools

import jax
import jax.numpy as jnp
from jax import lax
from jax.experimental import pallas as pl
from jax.experimental.pallas import tpu as pltpu
from jax.sharding import PartitionSpec as P

HD = 128
NEG = -1e30
LOG2E = 1.4426950408889634
MESH = pl.DeviceIdType.MESH


def kernel(
    group, pair, mp, heads, lead,
    lengths, query, key, value, out,
    q_buf, k_buf, v_buf, o_buf, first, p_buf, t_buf,
    q_in, k_in, v_in, o_in, q_out, k_out, v_out, o_out, first_in, ready,
):
    rows = query.shape[0]
    part = rows // mp
    per_core = heads // pair
    others = group // pair
    extra = lead * (others - 1)
    held = per_core - extra
    slots = lengths.shape[1]
    seq_index = lax.axis_index("seq")
    mp_index = lax.axis_index("mp")
    bucket = seq_index // group
    place = lax.rem(seq_index, group)
    core = lax.rem(place, pair)
    chip = place // pair

    def chip_at(chip_step):
        return lax.rem(chip + chip_step, others)

    def seq_of(chip_step, there_core):
        return bucket * group + chip_at(chip_step) * pair + there_core

    def head_of(slot, there_chip):
        if isinstance(slot, int) and slot < lead:
            return slot * others + there_chip
        return slot + extra

    def columns(owner, head):
        return pl.ds(pl.multiple_of((owner * per_core + head) * HD, HD), HD)

    def block_at(index):
        return pl.ds(pl.multiple_of(index * rows, rows), rows)

    kinds = ((query, q_buf, q_out, q_in), (key, k_buf, k_out, k_in), (value, v_buf, v_out, v_in))

    def local_copies(slot):
        mine = columns(core, head_of(slot, chip))
        return [
            pltpu.make_async_copy(source.at[:, mine], buf.at[slot, block_at(place), :], landed.at[slot, place])
            for source, buf, left, landed in kinds
        ]

    def far_kinds(slot):
        whole = isinstance(slot, int) and slot < lead
        return (0, 1, 2) if whole else (1, 2)

    far = [(chip_step, there_core) for there_core in range(pair) for chip_step in range(1, others)]

    def first_copies():
        return [
            pltpu.make_async_copy(
                kinds[kind][0].at[:, columns(there_core, head_of(0, chip_at(chip_step)))],
                first.at[kind, chip_step * pair + there_core],
                first_in.at[kind, chip_step * pair + there_core],
            )
            for kind in far_kinds(0) for chip_step, there_core in far
        ]

    def send(slot, chip_step, there_core, kind, staged=False):
        source, buf, left, landed = kinds[kind]
        index = chip_step * pair + there_core
        if staged:
            origin = first.at[kind, index]
        else:
            origin = source.at[:, columns(there_core, head_of(slot, chip_at(chip_step)))]
        return pltpu.make_async_remote_copy(
            src_ref=origin, dst_ref=buf.at[slot, block_at(place), :],
            send_sem=left.at[slot, index], recv_sem=landed.at[slot, place],
            device_id={"seq": seq_of(chip_step, there_core), "mp": mp_index}, device_id_type=MESH,
        )

    def far_sends(slot, staged=False):
        return [send(slot, a, b, kind, staged) for kind in far_kinds(slot) for a, b in far]

    def near_sends(slot):
        return [
            send(slot, 0, lax.rem(core + step, pair), kind)
            for kind in range(3) for step in range(1, pair)
        ]

    def result(turn, slot, chip_step, core_step, mp_step):
        there_core = lax.rem(core + core_step, pair)
        there_mp = lax.rem(mp_index + mp_step, mp)
        source = o_buf.at[turn, pl.ds(pl.multiple_of(there_core * rows + there_mp * part, part), part), :]
        column = (mp_index * heads + core * per_core + head_of(slot, chip)) * HD
        target = out.at[:, pl.ds(pl.multiple_of(column, HD), HD)]
        index = core_step * mp + mp_step
        if chip_step == 0 and index == 0:
            return pltpu.make_async_copy(source, target, o_in.at[turn, index])
        return pltpu.make_async_remote_copy(
            src_ref=source, dst_ref=target, send_sem=o_out.at[turn, index], recv_sem=o_in.at[turn, index],
            device_id={"seq": seq_of(chip_step, there_core), "mp": there_mp}, device_id_type=MESH,
        )

    for copy in first_copies():
        copy.start()

    barrier = pltpu.get_barrier_semaphore()
    beside = [(seq_of(0, b), lax.rem(mp_index + m, mp)) for b in range(pair) for m in range(1, mp)]
    greeted = [(seq_of(a, b), mp_index) for a, b in far]
    greeted += [(seq_of(0, lax.rem(core + b, pair)), mp_index) for b in range(1, pair)]
    greeted += beside
    for there_seq, there_mp in greeted:
        pl.semaphore_signal(
            barrier, inc=1, device_id={"seq": there_seq, "mp": there_mp}, device_id_type=MESH
        )

    for slot in range(max(lead, 1)):
        for copy in local_copies(slot):
            copy.start()

    @pl.loop(max(lead, 1), held)
    def _(slot):
        for copy in local_copies(slot):
            copy.start()

    ends = []
    running = jnp.int32(0)
    for i in range(slots):
        running = running + lengths[bucket, i]
        ends.append(running)

    def ids(offset):
        found = jnp.zeros_like(offset)
        for end in ends:
            found = found + (offset >= end).astype(jnp.int32)
        return found

    k_ids = ids(lax.broadcasted_iota(jnp.int32, (1, group * rows), 1))

    for copy in first_copies():
        copy.wait()
    pl.semaphore_wait(barrier, len(greeted))

    for slot in range(max(lead, 1)):
        for copy in far_sends(slot, slot == 0) + near_sends(slot):
            copy.start()

    @pl.loop(max(lead, 1), held)
    def _(slot):
        for copy in far_sends(slot) + near_sends(slot):
            copy.start()

    if lead:
        for there_seq, there_mp in beside:
            pl.semaphore_signal(
                ready, inc=1, device_id={"seq": there_seq, "mp": there_mp}, device_id_type=MESH
            )

    def arrived(kind, slot, base, count):
        buf, landed = kinds[kind][1], kinds[kind][3]
        for i in range(count):
            ref = buf.at[slot, block_at(base + i), :]
            pltpu.make_async_copy(ref, ref, landed.at[slot, base + i]).wait()

    factor = LOG2E / HD**0.5

    def weigh(slot, chip_step):
        keys = k_buf[slot]
        for b in range(pair):
            block = pl.ds(b * rows, rows)
            from_row = (chip_at(chip_step) * pair + b) * rows
            q_ids = ids(lax.broadcasted_iota(jnp.int32, (rows, 1), 0) + from_row)
            score = lax.dot_general(
                q_buf[slot, pl.ds(pl.multiple_of(from_row, rows), rows), :], keys,
                (((1,), (1,)), ((), ())), preferred_element_type=jnp.float32,
            )
            score = jnp.where(q_ids == k_ids, score, NEG)
            top = jnp.max(score, axis=1, keepdims=True)
            weight = jnp.exp2((score - top) * factor)
            t_buf[block, :] = jnp.broadcast_to(jnp.sum(weight, axis=1, keepdims=True), (rows, HD))
            p_buf[block, :] = weight.astype(jnp.bfloat16)

    def attend(turn, slot, chip_step):
        for core_step in reversed(range(pair)):
            block = block_at(lax.rem(core + core_step, pair))
            summed = jnp.dot(p_buf[block, :], v_buf[slot], preferred_element_type=jnp.float32)
            o_buf[turn, block, :] = (summed / t_buf[block, :]).astype(jnp.bfloat16)
            if chip_step == 0:
                for mp_step in reversed(range(mp)):
                    result(turn, slot, 0, core_step, mp_step).start()

    def far_results(mp_steps):
        return [
            result(slot * (others - 1) + a - 1, slot, a, core_step, mp_step)
            for slot in range(lead) for mp_step in mp_steps
            for core_step in range(pair) for a in range(1, others)
        ]

    def settle(turn, slot, chip_step=0):
        for core_step in range(pair):
            for mp_step in range(mp):
                copy = result(turn, slot, chip_step, core_step, mp_step)
                if chip_step == 0 and core_step == 0 and mp_step == 0:
                    copy.wait()
                else:
                    copy.wait_send()
                    copy.wait_recv()

    for slot in range(lead):
        arrived(0, slot, 0, group)
        arrived(1, slot, 0, group)
        for step in range(1, others):
            weigh(slot, step)
            if step == 1:
                arrived(2, slot, 0, group)
            attend(slot * (others - 1) + step - 1, slot, step)
        weigh(slot, 0)
        attend(slot + extra, slot, 0)
        for copy in far_sends(slot, slot == 0) + near_sends(slot):
            copy.wait_send()
    if lead:
        pl.semaphore_wait(ready, len(beside))
        for copy in far_results(list(range(1, mp)) + [0]):
            copy.start()

    @pl.loop(lead, held)
    def _(slot):
        arrived(0, slot, chip * pair, pair)
        arrived(1, slot, 0, group)
        weigh(slot, 0)
        arrived(2, slot, 0, group)
        attend(slot + extra, slot, 0)
        for copy in far_sends(slot) + near_sends(slot):
            copy.wait_send()

        @pl.when(slot > lead)
        def _():
            settle(slot + extra - 1, slot - 1)

    for slot in range(lead):
        settle(slot + extra, slot)
    settle(held - 1 + extra, held - 1)
    for slot in range(lead):
        for step in range(1, others):
            settle(slot * (others - 1) + step - 1, slot, step)


def duo(
    heads, pieces,
    lengths, query, key, value, out,
    kept, weights, totals, results, table,
    landed, sent, result_in, result_out, table_in, ready,
):
    rows = query.shape[0]
    mp = lax.axis_size("mp")
    part = rows // mp
    wide = heads // 4
    slots = lengths.shape[1]
    seq_index = lax.axis_index("seq")
    mp_index = lax.axis_index("mp")
    bucket = seq_index // 4
    place = lax.rem(seq_index, 4)
    core = lax.rem(place, 2)
    chip = place // 2
    other = 1 - chip
    inputs = (query, key, value)

    def device(there_chip, there_core, there_mp):
        return {"seq": bucket * 4 + there_chip * 2 + there_core, "mp": there_mp}

    def lanes(piece, base=0):
        first, count = pieces[piece]
        return pl.ds(pl.multiple_of((base + first) * HD, HD), count * HD)

    def block_at(index):
        return pl.ds(pl.multiple_of(index * rows, rows), rows)

    def send(kind, piece, there_chip, there_core):
        return pltpu.make_async_remote_copy(
            src_ref=inputs[kind].at[:, lanes(piece, (there_core * 2 + there_chip) * wide)],
            dst_ref=kept.at[kind, block_at(place), lanes(piece)],
            send_sem=sent, recv_sem=landed.at[kind, piece],
            device_id=device(there_chip, there_core, mp_index), device_id_type=MESH,
        )

    def keep(kind, piece):
        return pltpu.make_async_copy(
            inputs[kind].at[:, lanes(piece, (core * 2 + chip) * wide)],
            kept.at[kind, block_at(place), lanes(piece)], landed.at[kind, piece],
        )

    def result(piece, there_chip, core_step, mp_step):
        there_core = core_step if there_chip is other else lax.rem(core + core_step, 2)
        there_mp = lax.rem(mp_index + mp_step, mp)
        first = (there_chip * 2 + there_core) * rows + there_mp * part
        source = results.at[pl.ds(pl.multiple_of(first, part), part), lanes(piece)]
        target = out.at[:, lanes(piece, mp_index * heads + (core * 2 + chip) * wide)]
        if there_chip is chip and core_step == 0 and mp_step == 0:
            target[...] = source[...]
            return
        pltpu.make_async_remote_copy(
            src_ref=source, dst_ref=target, send_sem=result_out, recv_sem=result_in,
            device_id=device(there_chip, there_core, there_mp), device_id_type=MESH,
        ).start()

    barrier = pltpu.get_barrier_semaphore()
    far = [device(other, b, mp_index) for b in range(2)]
    beside = [device(chip, b, lax.rem(mp_index + m, mp)) for m in range(1, mp) for b in range(2)]

    def greet(semaphore, devices):
        for there in devices:
            pl.semaphore_signal(semaphore, inc=1, device_id=there, device_id_type=MESH)

    greet(barrier, far)
    root = jnp.logical_and(chip == 0, mp_index == 0)
    leaf = jnp.logical_and(chip == 0, mp_index != 0)
    rooted = [device(0, b, 0) for b in range(2)]
    pl.when(root)(lambda: greet(barrier, beside))
    pl.semaphore_wait(barrier, len(far) + lax.select(leaf, len(rooted), 0))

    for piece in range(len(pieces)):
        for kind in (1, 0, 2):
            for there_core in range(2):
                send(kind, piece, other, there_core).start()
    fetch = pltpu.make_async_copy(lengths, table, table_in)
    fetch.start()
    for piece in range(len(pieces)):
        for kind in (1, 0, 2):
            keep(kind, piece).start()

    greet(ready, far)

    pl.when(leaf)(lambda: greet(ready, rooted))

    @pl.when(root)
    def _():
        pl.semaphore_wait(ready, len(far) + len(beside))
        greet(ready, beside)

    pl.when(leaf)(lambda: pl.semaphore_wait(ready, len(far) + len(rooted)))
    pl.when(chip == 0)(lambda: greet(ready, far))

    pl.when(chip != 0)(lambda: pl.semaphore_wait(ready, 2 * len(far)))

    for piece in range(len(pieces)):
        for kind in (1, 0, 2):
            send(kind, piece, chip, 1 - core).start()

    fetch.wait()
    ends = []
    running = jnp.int32(0)
    for i in range(slots):
        running = running + table[bucket, i]
        ends.append(running)

    def ids(offset):
        found = jnp.zeros_like(offset)
        for end in ends:
            found = found + (offset >= end).astype(jnp.int32)
        return found

    k_ids = ids(lax.broadcasted_iota(jnp.int32, (1, 4 * rows), 1))
    factor = LOG2E / HD**0.5

    def arrived(kind, piece):
        ref = kept.at[kind, :, lanes(piece)]
        pltpu.make_async_copy(ref, ref, landed.at[kind, piece]).wait()

    def heads_of(piece):
        first, count = pieces[piece]
        return [(head, slice(head * HD, (head + 1) * HD)) for head in range(first, first + count)]

    def weigh(piece, index):
        block = block_at(index)
        q_ids = ids(lax.broadcasted_iota(jnp.int32, (rows, 1), 0) + index * rows)
        for head, lane in heads_of(piece):
            score = lax.dot_general(
                kept[0, block, lane], kept[1, :, lane],
                (((1,), (1,)), ((), ())), preferred_element_type=jnp.float32,
            )
            score = jnp.where(q_ids == k_ids, score, NEG)
            top = jnp.max(score, axis=1, keepdims=True)
            weight = jnp.exp2((score - top) * factor)
            totals[head, block, :] = jnp.broadcast_to(jnp.sum(weight, axis=1, keepdims=True), (rows, HD))
            weights[head, block, :] = weight.astype(jnp.bfloat16)

    def attend(piece, index, count=1):
        block = pl.ds(pl.multiple_of(index * count * rows, count * rows), count * rows)
        for head, lane in heads_of(piece):
            summed = jnp.dot(weights[head, block, :], kept[2, :, lane], preferred_element_type=jnp.float32)
            results[block, lane] = (summed / totals[head, block, :]).astype(jnp.bfloat16)

    def direct(piece):
        for core_step in range(2):
            result(piece, other, core_step, 0)

    def diagonal(piece, cores=(0, 1)):
        for mp_step in range(1, mp):
            for core_step in cores:
                result(piece, other, core_step, mp_step)

    def own(piece):
        for core_step in reversed(range(2)):
            for mp_step in reversed(range(mp)):
                result(piece, chip, core_step, mp_step)

    def each(work, piece, there_chip):
        @pl.loop(0, 2)
        def _(step):
            work(piece, there_chip * 2 + step)

    last = len(pieces) - 1
    for piece in range(len(pieces)):
        arrived(1, piece)
        arrived(0, piece)
        each(weigh, piece, other)
        if piece < last:
            each(weigh, piece, chip)
        if piece:
            both = jnp.logical_and(mp_index == 1, chip == 1)
            pl.when(mp_index == 1)(lambda: diagonal(piece - 1, (0,)))
            pl.when(both)(lambda: diagonal(piece - 1, (1,)))
        if piece == last:
            each(weigh, piece, chip)
        arrived(2, piece)
        if piece:
            pl.when(mp_index != 1)(lambda: diagonal(piece - 1, (0,)))
            pl.when(jnp.logical_not(both))(lambda: diagonal(piece - 1, (1,)))
        if piece == last:
            attend(piece, other, 2)
        else:
            each(attend, piece, other)
        if piece == last:
            diagonal(piece)
        direct(piece)
        each(attend, piece, chip)
        own(piece)

    whole = kept.at[:, pl.ds(0, 3 * rows)]
    pltpu.make_async_copy(whole, whole, sent).wait()
    moved = out.at[:, pl.ds(0, out.shape[1] - wide * HD)]
    pltpu.make_async_copy(moved, moved, result_out).wait()
    pltpu.make_async_copy(moved, moved, result_in).wait()


def duo_call(query, key, value, clip_lengths):
    rows, width = query.shape
    heads = width // HD
    mp = lax.axis_size("mp")
    wide = heads // 4
    early = (wide + 1) // 2
    pieces = [(0, early)] + [(head, 1) for head in range(early, wide)]
    dma = pltpu.SemaphoreType.DMA
    whole = pl.BlockSpec(memory_space=pl.ANY)
    return pl.pallas_call(
        functools.partial(duo, heads, pieces),
        out_shape=pltpu.VMEM((rows // mp, width * mp), jnp.bfloat16),
        in_specs=[whole] * 4,
        out_specs=pl.BlockSpec(memory_space=pltpu.VMEM),
        scratch_shapes=[
            pltpu.VMEM((3, 4 * rows, wide * HD), jnp.bfloat16),
            pltpu.VMEM((wide, 4 * rows, 4 * rows), jnp.bfloat16),
            pltpu.VMEM((wide, 4 * rows, HD), jnp.float32),
            pltpu.VMEM((4 * rows, wide * HD), jnp.bfloat16),
            pltpu.SMEM(clip_lengths.shape, jnp.int32),
            dma((3, len(pieces))), dma(()), dma(()), dma(()), dma(()), pltpu.SemaphoreType.REGULAR,
        ],
        compiler_params=pltpu.CompilerParams(collective_id=0, has_side_effects=True),
        name="packed_attention",
    )(clip_lengths, query, key, value)


def shards(query, key, value, clip_lengths):
    rows, width = query.shape
    heads = width // HD
    group = lax.axis_size("seq") // clip_lengths.shape[0]
    mp = lax.axis_size("mp")
    if group == 4 and heads % 4 == 0 and rows % (16 * mp) == 0 and mp > 1:
        return duo_call(query, key, value, clip_lengths)
    pair = 2 if group % 2 == 0 and heads % 2 == 0 else 1
    per_core = heads // pair
    others = group // pair
    lead = min(2, (per_core - 1) // others) if others > 1 else 0
    held = per_core - lead * (others - 1)
    dma = pltpu.SemaphoreType.DMA
    whole = pl.BlockSpec(memory_space=pl.ANY)
    return pl.pallas_call(
        functools.partial(kernel, group, pair, mp, heads, lead),
        out_shape=pltpu.VMEM((rows // mp, width * mp), jnp.bfloat16),
        in_specs=[pl.BlockSpec(memory_space=pltpu.SMEM), whole, whole, whole],
        out_specs=pl.BlockSpec(memory_space=pltpu.VMEM),
        scratch_shapes=[
            pltpu.VMEM((held, group * rows, HD), jnp.bfloat16),
            pltpu.VMEM((held, group * rows, HD), jnp.bfloat16),
            pltpu.VMEM((held, group * rows, HD), jnp.bfloat16),
            pltpu.VMEM((per_core, pair * rows, HD), jnp.bfloat16),
            pltpu.VMEM((3, group, rows, HD), jnp.bfloat16),
            pltpu.VMEM((pair * rows, group * rows), jnp.bfloat16),
            pltpu.VMEM((pair * rows, HD), jnp.float32),
            dma((held, group)), dma((held, group)), dma((held, group)), dma((per_core, pair * mp)),
            dma((held, group)), dma((held, group)), dma((held, group)), dma((per_core, pair * mp)),
            dma((3, group)), pltpu.SemaphoreType.REGULAR,
        ],
        compiler_params=pltpu.CompilerParams(collective_id=0, has_side_effects=True),
        name="packed_attention",
    )(clip_lengths, query, key, value)


def solution(mesh):
    in_specs = (P("seq", "mp"), P("seq", "mp"), P("seq", "mp"), P())
    out_specs = P(("seq", "mp"), None)
    return jax.shard_map(shards, mesh=mesh, in_specs=in_specs, out_specs=out_specs, check_vma=False)
```

```python
import functools

import jax
import jax.numpy as jnp
from jax import lax
from jax.experimental import pallas as pl
from jax.experimental.pallas import tpu as pltpu
from jax.sharding import PartitionSpec as P

HD = 128
NEG = -1e30
LOG2E = 1.4426950408889634
MESH = pl.DeviceIdType.MESH


def kernel(
    group, pair, mp, heads, lead,
    lengths, query, key, value, out,
    q_buf, k_buf, v_buf, o_buf, first, p_buf, t_buf,
    q_in, k_in, v_in, o_in, q_out, k_out, v_out, o_out, first_in, ready,
):
    rows = query.shape[0]
    part = rows // mp
    per_core = heads // pair
    others = group // pair
    extra = lead * (others - 1)
    held = per_core - extra
    slots = lengths.shape[1]
    seq_index = lax.axis_index("seq")
    mp_index = lax.axis_index("mp")
    bucket = seq_index // group
    place = lax.rem(seq_index, group)
    core = lax.rem(place, pair)
    chip = place // pair

    def chip_at(chip_step):
        return lax.rem(chip + chip_step, others)

    def seq_of(chip_step, there_core):
        return bucket * group + chip_at(chip_step) * pair + there_core

    def head_of(slot, there_chip):
        if isinstance(slot, int) and slot < lead:
            return slot * others + there_chip
        return slot + extra

    def columns(owner, head):
        return pl.ds(pl.multiple_of((owner * per_core + head) * HD, HD), HD)

    def block_at(index):
        return pl.ds(pl.multiple_of(index * rows, rows), rows)

    kinds = ((query, q_buf, q_out, q_in), (key, k_buf, k_out, k_in), (value, v_buf, v_out, v_in))

    def local_copies(slot):
        mine = columns(core, head_of(slot, chip))
        return [
            pltpu.make_async_copy(source.at[:, mine], buf.at[slot, block_at(place), :], landed.at[slot, place])
            for source, buf, left, landed in kinds
        ]

    def far_kinds(slot):
        whole = isinstance(slot, int) and slot < lead
        return (0, 1, 2) if whole else (1, 2)

    far = [(chip_step, there_core) for there_core in range(pair) for chip_step in range(1, others)]

    def first_copies():
        return [
            pltpu.make_async_copy(
                kinds[kind][0].at[:, columns(there_core, head_of(0, chip_at(chip_step)))],
                first.at[kind, chip_step * pair + there_core],
                first_in.at[kind, chip_step * pair + there_core],
            )
            for kind in far_kinds(0) for chip_step, there_core in far
        ]

    def send(slot, chip_step, there_core, kind, staged=False):
        source, buf, left, landed = kinds[kind]
        index = chip_step * pair + there_core
        if staged:
            origin = first.at[kind, index]
        else:
            origin = source.at[:, columns(there_core, head_of(slot, chip_at(chip_step)))]
        return pltpu.make_async_remote_copy(
            src_ref=origin, dst_ref=buf.at[slot, block_at(place), :],
            send_sem=left.at[slot, index], recv_sem=landed.at[slot, place],
            device_id={"seq": seq_of(chip_step, there_core), "mp": mp_index}, device_id_type=MESH,
        )

    def far_sends(slot, staged=False):
        return [send(slot, a, b, kind, staged) for kind in far_kinds(slot) for a, b in far]

    def near_sends(slot):
        return [
            send(slot, 0, lax.rem(core + step, pair), kind)
            for kind in range(3) for step in range(1, pair)
        ]

    def result(turn, slot, chip_step, core_step, mp_step):
        there_core = lax.rem(core + core_step, pair)
        there_mp = lax.rem(mp_index + mp_step, mp)
        source = o_buf.at[turn, pl.ds(pl.multiple_of(there_core * rows + there_mp * part, part), part), :]
        column = (mp_index * heads + core * per_core + head_of(slot, chip)) * HD
        target = out.at[:, pl.ds(pl.multiple_of(column, HD), HD)]
        index = core_step * mp + mp_step
        if chip_step == 0 and index == 0:
            return pltpu.make_async_copy(source, target, o_in.at[turn, index])
        return pltpu.make_async_remote_copy(
            src_ref=source, dst_ref=target, send_sem=o_out.at[turn, index], recv_sem=o_in.at[turn, index],
            device_id={"seq": seq_of(chip_step, there_core), "mp": there_mp}, device_id_type=MESH,
        )

    for copy in first_copies():
        copy.start()

    barrier = pltpu.get_barrier_semaphore()
    beside = [(seq_of(0, b), lax.rem(mp_index + m, mp)) for b in range(pair) for m in range(1, mp)]
    greeted = [(seq_of(a, b), mp_index) for a, b in far]
    greeted += [(seq_of(0, lax.rem(core + b, pair)), mp_index) for b in range(1, pair)]
    greeted += beside
    for there_seq, there_mp in greeted:
        pl.semaphore_signal(
            barrier, inc=1, device_id={"seq": there_seq, "mp": there_mp}, device_id_type=MESH
        )

    for slot in range(max(lead, 1)):
        for copy in local_copies(slot):
            copy.start()

    @pl.loop(max(lead, 1), held)
    def _(slot):
        for copy in local_copies(slot):
            copy.start()

    ends = []
    running = jnp.int32(0)
    for i in range(slots):
        running = running + lengths[bucket, i]
        ends.append(running)

    def ids(offset):
        found = jnp.zeros_like(offset)
        for end in ends:
            found = found + (offset >= end).astype(jnp.int32)
        return found

    k_ids = ids(lax.broadcasted_iota(jnp.int32, (1, group * rows), 1))

    for copy in first_copies():
        copy.wait()
    pl.semaphore_wait(barrier, len(greeted))

    for slot in range(max(lead, 1)):
        for copy in far_sends(slot, slot == 0) + near_sends(slot):
            copy.start()

    @pl.loop(max(lead, 1), held)
    def _(slot):
        for copy in far_sends(slot) + near_sends(slot):
            copy.start()

    if lead:
        for there_seq, there_mp in beside:
            pl.semaphore_signal(
                ready, inc=1, device_id={"seq": there_seq, "mp": there_mp}, device_id_type=MESH
            )

    def arrived(kind, slot, base, count):
        buf, landed = kinds[kind][1], kinds[kind][3]
        for i in range(count):
            ref = buf.at[slot, block_at(base + i), :]
            pltpu.make_async_copy(ref, ref, landed.at[slot, base + i]).wait()

    factor = LOG2E / HD**0.5

    def weigh(slot, chip_step):
        keys = k_buf[slot]
        for b in range(pair):
            block = pl.ds(b * rows, rows)
            from_row = (chip_at(chip_step) * pair + b) * rows
            q_ids = ids(lax.broadcasted_iota(jnp.int32, (rows, 1), 0) + from_row)
            score = lax.dot_general(
                q_buf[slot, pl.ds(pl.multiple_of(from_row, rows), rows), :], keys,
                (((1,), (1,)), ((), ())), preferred_element_type=jnp.float32,
            )
            score = jnp.where(q_ids == k_ids, score, NEG)
            top = jnp.max(score, axis=1, keepdims=True)
            weight = jnp.exp2((score - top) * factor)
            t_buf[block, :] = jnp.broadcast_to(jnp.sum(weight, axis=1, keepdims=True), (rows, HD))
            p_buf[block, :] = weight.astype(jnp.bfloat16)

    def attend(turn, slot, chip_step):
        for core_step in reversed(range(pair)):
            block = block_at(lax.rem(core + core_step, pair))
            summed = jnp.dot(p_buf[block, :], v_buf[slot], preferred_element_type=jnp.float32)
            o_buf[turn, block, :] = (summed / t_buf[block, :]).astype(jnp.bfloat16)
            if chip_step == 0:
                for mp_step in reversed(range(mp)):
                    result(turn, slot, 0, core_step, mp_step).start()

    def far_results(mp_steps):
        return [
            result(slot * (others - 1) + a - 1, slot, a, core_step, mp_step)
            for slot in range(lead) for mp_step in mp_steps
            for core_step in range(pair) for a in range(1, others)
        ]

    def settle(turn, slot, chip_step=0):
        for core_step in range(pair):
            for mp_step in range(mp):
                copy = result(turn, slot, chip_step, core_step, mp_step)
                if chip_step == 0 and core_step == 0 and mp_step == 0:
                    copy.wait()
                else:
                    copy.wait_send()
                    copy.wait_recv()

    for slot in range(lead):
        arrived(0, slot, 0, group)
        arrived(1, slot, 0, group)
        for step in range(1, others):
            weigh(slot, step)
            if step == 1:
                arrived(2, slot, 0, group)
            attend(slot * (others - 1) + step - 1, slot, step)
        weigh(slot, 0)
        attend(slot + extra, slot, 0)
        for copy in far_sends(slot, slot == 0) + near_sends(slot):
            copy.wait_send()
    if lead:
        pl.semaphore_wait(ready, len(beside))
        for copy in far_results(list(range(1, mp)) + [0]):
            copy.start()

    @pl.loop(lead, held)
    def _(slot):
        arrived(0, slot, chip * pair, pair)
        arrived(1, slot, 0, group)
        weigh(slot, 0)
        arrived(2, slot, 0, group)
        attend(slot + extra, slot, 0)
        for copy in far_sends(slot) + near_sends(slot):
            copy.wait_send()

        @pl.when(slot > lead)
        def _():
            settle(slot + extra - 1, slot - 1)

    for slot in range(lead):
        settle(slot + extra, slot)
    settle(held - 1 + extra, held - 1)
    for slot in range(lead):
        for step in range(1, others):
            settle(slot * (others - 1) + step - 1, slot, step)


def duo(
    heads, pieces,
    lengths, query, key, value, out,
    kept, weights, totals, results, table,
    landed, sent, result_in, table_in, ready,
):
    rows = query.shape[0]
    mp = lax.axis_size("mp")
    part = rows // mp
    wide = heads // 4
    slots = lengths.shape[1]
    seq_index = lax.axis_index("seq")
    mp_index = lax.axis_index("mp")
    bucket = seq_index // 4
    place = lax.rem(seq_index, 4)
    core = lax.rem(place, 2)
    chip = place // 2
    other = 1 - chip
    inputs = (query, key, value)

    def device(there_chip, there_core, there_mp):
        return {"seq": bucket * 4 + there_chip * 2 + there_core, "mp": there_mp}

    def lanes(piece, base=0):
        first, count = pieces[piece]
        return pl.ds(pl.multiple_of((base + first) * HD, HD), count * HD)

    def block_at(index):
        return pl.ds(pl.multiple_of(index * rows, rows), rows)

    def send(kind, piece, there_chip, there_core):
        return pltpu.make_async_remote_copy(
            src_ref=inputs[kind].at[:, lanes(piece, (there_core * 2 + there_chip) * wide)],
            dst_ref=kept.at[kind, block_at(place), lanes(piece)],
            send_sem=sent, recv_sem=landed.at[kind // 2, piece],
            device_id=device(there_chip, there_core, mp_index), device_id_type=MESH,
        )

    def keep(kind, piece):
        return pltpu.make_async_copy(
            inputs[kind].at[:, lanes(piece, (core * 2 + chip) * wide)],
            kept.at[kind, block_at(place), lanes(piece)], landed.at[kind // 2, piece],
        )

    def result(piece, there_chip, core_step, mp_step):
        there_core = core_step if there_chip is other else lax.rem(core + core_step, 2)
        there_mp = lax.rem(mp_index + mp_step, mp)
        first = (there_chip * 2 + there_core) * rows + there_mp * part
        source = results.at[pl.ds(pl.multiple_of(first, part), part), lanes(piece)]
        target = out.at[:, lanes(piece, mp_index * heads + (core * 2 + chip) * wide)]
        if there_chip is chip and core_step == 0 and mp_step == 0:
            target[...] = source[...]
            return
        pltpu.make_async_remote_copy(
            src_ref=source, dst_ref=target, send_sem=sent, recv_sem=result_in,
            device_id=device(there_chip, there_core, there_mp), device_id_type=MESH,
        ).start()

    barrier = pltpu.get_barrier_semaphore()
    far = [device(other, b, mp_index) for b in range(2)]
    beside = [device(chip, b, lax.rem(mp_index + m, mp)) for m in range(1, mp) for b in range(2)]

    def greet(semaphore, devices):
        for there in devices:
            pl.semaphore_signal(semaphore, inc=1, device_id=there, device_id_type=MESH)

    greet(barrier, far)
    root = jnp.logical_and(chip == 0, mp_index == 0)
    leaf = jnp.logical_and(chip == 0, mp_index != 0)
    rooted = [device(0, b, 0) for b in range(2)]
    pl.when(root)(lambda: greet(barrier, beside))
    pl.semaphore_wait(barrier, len(far) + lax.select(leaf, len(rooted), 0))

    for piece in range(len(pieces)):
        for kind in (1, 0, 2):
            for there_core in range(2):
                send(kind, piece, other, there_core).start()
    fetch = pltpu.make_async_copy(lengths, table, table_in)
    fetch.start()
    for piece in range(len(pieces)):
        for kind in (1, 0, 2):
            keep(kind, piece).start()

    greet(ready, far)

    pl.when(leaf)(lambda: greet(ready, rooted))

    @pl.when(root)
    def _():
        pl.semaphore_wait(ready, len(far) + len(beside))
        greet(ready, beside)

    pl.when(leaf)(lambda: pl.semaphore_wait(ready, len(far) + len(rooted)))
    pl.when(chip == 0)(lambda: greet(ready, far))

    pl.when(chip != 0)(lambda: pl.semaphore_wait(ready, 2 * len(far)))

    for piece in range(len(pieces)):
        for kind in (1, 0, 2):
            send(kind, piece, chip, 1 - core).start()

    fetch.wait()
    ends = []
    running = jnp.int32(0)
    for i in range(slots):
        running = running + table[bucket, i]
        ends.append(running)

    def ids(offset):
        found = jnp.zeros_like(offset)
        for end in ends:
            found = found + (offset >= end).astype(jnp.int32)
        return found

    k_ids = ids(lax.broadcasted_iota(jnp.int32, (1, 4 * rows), 1))
    factor = LOG2E / HD**0.5

    def arrived(kind, piece):
        ref = kept.at[2 if kind == 2 else pl.ds(0, 2), :, lanes(piece)]
        pltpu.make_async_copy(ref, ref, landed.at[kind // 2, piece]).wait()

    def heads_of(piece):
        first, count = pieces[piece]
        return [(head, slice(head * HD, (head + 1) * HD)) for head in range(first, first + count)]

    def weigh(piece, index):
        block = block_at(index)
        q_ids = ids(lax.broadcasted_iota(jnp.int32, (rows, 1), 0) + index * rows)
        for head, lane in heads_of(piece):
            score = lax.dot_general(
                kept[0, block, lane], kept[1, :, lane],
                (((1,), (1,)), ((), ())), preferred_element_type=jnp.float32,
            )
            score = jnp.where(q_ids == k_ids, score, NEG)
            top = jnp.max(score, axis=1, keepdims=True)
            weight = jnp.exp2((score - top) * factor)
            totals[head, block, :] = jnp.broadcast_to(jnp.sum(weight, axis=1, keepdims=True), (rows, HD))
            weights[head, block, :] = weight.astype(jnp.bfloat16)

    def attend(piece, index, count=1):
        block = pl.ds(pl.multiple_of(index * count * rows, count * rows), count * rows)
        for head, lane in heads_of(piece):
            summed = jnp.dot(weights[head, block, :], kept[2, :, lane], preferred_element_type=jnp.float32)
            results[block, lane] = (summed / totals[head, block, :]).astype(jnp.bfloat16)

    def direct(piece):
        for core_step in range(2):
            result(piece, other, core_step, 0)

    def diagonal(piece, cores=(0, 1)):
        for mp_step in range(1, mp):
            for core_step in cores:
                result(piece, other, core_step, mp_step)

    def own(piece):
        for core_step in reversed(range(2)):
            for mp_step in reversed(range(mp)):
                result(piece, chip, core_step, mp_step)

    def each(work, piece, there_chip):
        @pl.loop(0, 2)
        def _(step):
            work(piece, there_chip * 2 + step)

    last = len(pieces) - 1
    for piece in range(len(pieces)):
        arrived(0, piece)
        each(weigh, piece, other)
        if piece < last:
            each(weigh, piece, chip)
        if piece:
            both = jnp.logical_and(mp_index == 1, chip == 1)
            pl.when(mp_index == 1)(lambda: diagonal(piece - 1, (0,)))
            pl.when(both)(lambda: diagonal(piece - 1, (1,)))
        if piece == last:
            each(weigh, piece, chip)
        arrived(2, piece)
        if piece:
            pl.when(mp_index != 1)(lambda: diagonal(piece - 1, (0,)))
            pl.when(jnp.logical_not(both))(lambda: diagonal(piece - 1, (1,)))
        if piece == last:
            attend(piece, other, 2)
        else:
            each(attend, piece, other)
        direct(piece)
        if piece == last:
            diagonal(piece)
        each(attend, piece, chip)
        own(piece)

    whole = kept.at[:, pl.ds(0, 3 * rows)]
    pltpu.make_async_copy(whole, whole, sent).wait()
    moved = out.at[:, pl.ds(0, out.shape[1] - wide * HD)]
    pltpu.make_async_copy(moved, moved, sent).wait()
    pltpu.make_async_copy(moved, moved, result_in).wait()


def duo_call(query, key, value, clip_lengths):
    rows, width = query.shape
    heads = width // HD
    mp = lax.axis_size("mp")
    wide = heads // 4
    early = (wide + 1) // 2
    pieces = [(0, early)] + [(head, 1) for head in range(early, wide)]
    dma = pltpu.SemaphoreType.DMA
    whole = pl.BlockSpec(memory_space=pl.ANY)
    return pl.pallas_call(
        functools.partial(duo, heads, pieces),
        out_shape=pltpu.VMEM((rows // mp, width * mp), jnp.bfloat16),
        in_specs=[whole] * 4,
        out_specs=pl.BlockSpec(memory_space=pltpu.VMEM),
        scratch_shapes=[
            pltpu.VMEM((3, 4 * rows, wide * HD), jnp.bfloat16),
            pltpu.VMEM((wide, 4 * rows, 4 * rows), jnp.bfloat16),
            pltpu.VMEM((wide, 4 * rows, HD), jnp.float32),
            pltpu.VMEM((4 * rows, wide * HD), jnp.bfloat16),
            pltpu.SMEM(clip_lengths.shape, jnp.int32),
            dma((2, len(pieces))), dma(()), dma(()), dma(()), pltpu.SemaphoreType.REGULAR,
        ],
        compiler_params=pltpu.CompilerParams(collective_id=0, has_side_effects=True),
        name="packed_attention",
    )(clip_lengths, query, key, value)


def shards(query, key, value, clip_lengths):
    rows, width = query.shape
    heads = width // HD
    group = lax.axis_size("seq") // clip_lengths.shape[0]
    mp = lax.axis_size("mp")
    if group == 4 and heads % 4 == 0 and rows % (16 * mp) == 0 and mp > 1:
        return duo_call(query, key, value, clip_lengths)
    pair = 2 if group % 2 == 0 and heads % 2 == 0 else 1
    per_core = heads // pair
    others = group // pair
    lead = min(2, (per_core - 1) // others) if others > 1 else 0
    held = per_core - lead * (others - 1)
    dma = pltpu.SemaphoreType.DMA
    whole = pl.BlockSpec(memory_space=pl.ANY)
    return pl.pallas_call(
        functools.partial(kernel, group, pair, mp, heads, lead),
        out_shape=pltpu.VMEM((rows // mp, width * mp), jnp.bfloat16),
        in_specs=[pl.BlockSpec(memory_space=pltpu.SMEM), whole, whole, whole],
        out_specs=pl.BlockSpec(memory_space=pltpu.VMEM),
        scratch_shapes=[
            pltpu.VMEM((held, group * rows, HD), jnp.bfloat16),
            pltpu.VMEM((held, group * rows, HD), jnp.bfloat16),
            pltpu.VMEM((held, group * rows, HD), jnp.bfloat16),
            pltpu.VMEM((per_core, pair * rows, HD), jnp.bfloat16),
            pltpu.VMEM((3, group, rows, HD), jnp.bfloat16),
            pltpu.VMEM((pair * rows, group * rows), jnp.bfloat16),
            pltpu.VMEM((pair * rows, HD), jnp.float32),
            dma((held, group)), dma((held, group)), dma((held, group)), dma((per_core, pair * mp)),
            dma((held, group)), dma((held, group)), dma((held, group)), dma((per_core, pair * mp)),
            dma((3, group)), pltpu.SemaphoreType.REGULAR,
        ],
        compiler_params=pltpu.CompilerParams(collective_id=0, has_side_effects=True),
        name="packed_attention",
    )(clip_lengths, query, key, value)


def solution(mesh):
    in_specs = (P("seq", "mp"), P("seq", "mp"), P("seq", "mp"), P())
    out_specs = P(("seq", "mp"), None)
    return jax.shard_map(shards, mesh=mesh, in_specs=in_specs, out_specs=out_specs, check_vma=False)
```

```python
import functools

import jax
import jax.numpy as jnp
from jax import lax
from jax.experimental import pallas as pl
from jax.experimental.pallas import tpu as pltpu
from jax.sharding import PartitionSpec as P

HD = 128
NEG = -1e30
LOG2E = 1.4426950408889634
MESH = pl.DeviceIdType.MESH


def kernel(
    group, pair, mp, heads, lead,
    lengths, query, key, value, out,
    q_buf, k_buf, v_buf, o_buf, first, p_buf, t_buf,
    q_in, k_in, v_in, o_in, q_out, k_out, v_out, o_out, first_in, ready,
):
    rows = query.shape[0]
    part = rows // mp
    per_core = heads // pair
    others = group // pair
    extra = lead * (others - 1)
    held = per_core - extra
    slots = lengths.shape[1]
    seq_index = lax.axis_index("seq")
    mp_index = lax.axis_index("mp")
    bucket = seq_index // group
    place = lax.rem(seq_index, group)
    core = lax.rem(place, pair)
    chip = place // pair

    def chip_at(chip_step):
        return lax.rem(chip + chip_step, others)

    def seq_of(chip_step, there_core):
        return bucket * group + chip_at(chip_step) * pair + there_core

    def head_of(slot, there_chip):
        if isinstance(slot, int) and slot < lead:
            return slot * others + there_chip
        return slot + extra

    def columns(owner, head):
        return pl.ds(pl.multiple_of((owner * per_core + head) * HD, HD), HD)

    def block_at(index):
        return pl.ds(pl.multiple_of(index * rows, rows), rows)

    kinds = ((query, q_buf, q_out, q_in), (key, k_buf, k_out, k_in), (value, v_buf, v_out, v_in))

    def local_copies(slot):
        mine = columns(core, head_of(slot, chip))
        return [
            pltpu.make_async_copy(source.at[:, mine], buf.at[slot, block_at(place), :], landed.at[slot, place])
            for source, buf, left, landed in kinds
        ]

    def far_kinds(slot):
        whole = isinstance(slot, int) and slot < lead
        return (0, 1, 2) if whole else (1, 2)

    far = [(chip_step, there_core) for there_core in range(pair) for chip_step in range(1, others)]

    def first_copies():
        return [
            pltpu.make_async_copy(
                kinds[kind][0].at[:, columns(there_core, head_of(0, chip_at(chip_step)))],
                first.at[kind, chip_step * pair + there_core],
                first_in.at[kind, chip_step * pair + there_core],
            )
            for kind in far_kinds(0) for chip_step, there_core in far
        ]

    def send(slot, chip_step, there_core, kind, staged=False):
        source, buf, left, landed = kinds[kind]
        index = chip_step * pair + there_core
        if staged:
            origin = first.at[kind, index]
        else:
            origin = source.at[:, columns(there_core, head_of(slot, chip_at(chip_step)))]
        return pltpu.make_async_remote_copy(
            src_ref=origin, dst_ref=buf.at[slot, block_at(place), :],
            send_sem=left.at[slot, index], recv_sem=landed.at[slot, place],
            device_id={"seq": seq_of(chip_step, there_core), "mp": mp_index}, device_id_type=MESH,
        )

    def far_sends(slot, staged=False):
        return [send(slot, a, b, kind, staged) for kind in far_kinds(slot) for a, b in far]

    def near_sends(slot):
        return [
            send(slot, 0, lax.rem(core + step, pair), kind)
            for kind in range(3) for step in range(1, pair)
        ]

    def result(turn, slot, chip_step, core_step, mp_step):
        there_core = lax.rem(core + core_step, pair)
        there_mp = lax.rem(mp_index + mp_step, mp)
        source = o_buf.at[turn, pl.ds(pl.multiple_of(there_core * rows + there_mp * part, part), part), :]
        column = (mp_index * heads + core * per_core + head_of(slot, chip)) * HD
        target = out.at[:, pl.ds(pl.multiple_of(column, HD), HD)]
        index = core_step * mp + mp_step
        if chip_step == 0 and index == 0:
            return pltpu.make_async_copy(source, target, o_in.at[turn, index])
        return pltpu.make_async_remote_copy(
            src_ref=source, dst_ref=target, send_sem=o_out.at[turn, index], recv_sem=o_in.at[turn, index],
            device_id={"seq": seq_of(chip_step, there_core), "mp": there_mp}, device_id_type=MESH,
        )

    for copy in first_copies():
        copy.start()

    barrier = pltpu.get_barrier_semaphore()
    beside = [(seq_of(0, b), lax.rem(mp_index + m, mp)) for b in range(pair) for m in range(1, mp)]
    greeted = [(seq_of(a, b), mp_index) for a, b in far]
    greeted += [(seq_of(0, lax.rem(core + b, pair)), mp_index) for b in range(1, pair)]
    greeted += beside
    for there_seq, there_mp in greeted:
        pl.semaphore_signal(
            barrier, inc=1, device_id={"seq": there_seq, "mp": there_mp}, device_id_type=MESH
        )

    for slot in range(max(lead, 1)):
        for copy in local_copies(slot):
            copy.start()

    @pl.loop(max(lead, 1), held)
    def _(slot):
        for copy in local_copies(slot):
            copy.start()

    ends = []
    running = jnp.int32(0)
    for i in range(slots):
        running = running + lengths[bucket, i]
        ends.append(running)

    def ids(offset):
        found = jnp.zeros_like(offset)
        for end in ends:
            found = found + (offset >= end).astype(jnp.int32)
        return found

    k_ids = ids(lax.broadcasted_iota(jnp.int32, (1, group * rows), 1))

    for copy in first_copies():
        copy.wait()
    pl.semaphore_wait(barrier, len(greeted))

    for slot in range(max(lead, 1)):
        for copy in far_sends(slot, slot == 0) + near_sends(slot):
            copy.start()

    @pl.loop(max(lead, 1), held)
    def _(slot):
        for copy in far_sends(slot) + near_sends(slot):
            copy.start()

    if lead:
        for there_seq, there_mp in beside:
            pl.semaphore_signal(
                ready, inc=1, device_id={"seq": there_seq, "mp": there_mp}, device_id_type=MESH
            )

    def arrived(kind, slot, base, count):
        buf, landed = kinds[kind][1], kinds[kind][3]
        for i in range(count):
            ref = buf.at[slot, block_at(base + i), :]
            pltpu.make_async_copy(ref, ref, landed.at[slot, base + i]).wait()

    factor = LOG2E / HD**0.5

    def weigh(slot, chip_step):
        keys = k_buf[slot]
        for b in range(pair):
            block = pl.ds(b * rows, rows)
            from_row = (chip_at(chip_step) * pair + b) * rows
            q_ids = ids(lax.broadcasted_iota(jnp.int32, (rows, 1), 0) + from_row)
            score = lax.dot_general(
                q_buf[slot, pl.ds(pl.multiple_of(from_row, rows), rows), :], keys,
                (((1,), (1,)), ((), ())), preferred_element_type=jnp.float32,
            )
            score = jnp.where(q_ids == k_ids, score, NEG)
            top = jnp.max(score, axis=1, keepdims=True)
            weight = jnp.exp2((score - top) * factor)
            t_buf[block, :] = jnp.broadcast_to(jnp.sum(weight, axis=1, keepdims=True), (rows, HD))
            p_buf[block, :] = weight.astype(jnp.bfloat16)

    def attend(turn, slot, chip_step):
        for core_step in reversed(range(pair)):
            block = block_at(lax.rem(core + core_step, pair))
            summed = jnp.dot(p_buf[block, :], v_buf[slot], preferred_element_type=jnp.float32)
            o_buf[turn, block, :] = (summed / t_buf[block, :]).astype(jnp.bfloat16)
            if chip_step == 0:
                for mp_step in reversed(range(mp)):
                    result(turn, slot, 0, core_step, mp_step).start()

    def far_results(mp_steps):
        return [
            result(slot * (others - 1) + a - 1, slot, a, core_step, mp_step)
            for slot in range(lead) for mp_step in mp_steps
            for core_step in range(pair) for a in range(1, others)
        ]

    def settle(turn, slot, chip_step=0):
        for core_step in range(pair):
            for mp_step in range(mp):
                copy = result(turn, slot, chip_step, core_step, mp_step)
                if chip_step == 0 and core_step == 0 and mp_step == 0:
                    copy.wait()
                else:
                    copy.wait_send()
                    copy.wait_recv()

    for slot in range(lead):
        arrived(0, slot, 0, group)
        arrived(1, slot, 0, group)
        for step in range(1, others):
            weigh(slot, step)
            if step == 1:
                arrived(2, slot, 0, group)
            attend(slot * (others - 1) + step - 1, slot, step)
        weigh(slot, 0)
        attend(slot + extra, slot, 0)
        for copy in far_sends(slot, slot == 0) + near_sends(slot):
            copy.wait_send()
    if lead:
        pl.semaphore_wait(ready, len(beside))
        for copy in far_results(list(range(1, mp)) + [0]):
            copy.start()

    @pl.loop(lead, held)
    def _(slot):
        arrived(0, slot, chip * pair, pair)
        arrived(1, slot, 0, group)
        weigh(slot, 0)
        arrived(2, slot, 0, group)
        attend(slot + extra, slot, 0)
        for copy in far_sends(slot) + near_sends(slot):
            copy.wait_send()

        @pl.when(slot > lead)
        def _():
            settle(slot + extra - 1, slot - 1)

    for slot in range(lead):
        settle(slot + extra, slot)
    settle(held - 1 + extra, held - 1)
    for slot in range(lead):
        for step in range(1, others):
            settle(slot * (others - 1) + step - 1, slot, step)


def duo(
    heads, pieces,
    lengths, query, key, value, out,
    kept, weights, totals, results, table,
    landed, sent, result_in, result_out, table_in, ready,
):
    rows = query.shape[0]
    mp = lax.axis_size("mp")
    part = rows // mp
    wide = heads // 4
    slots = lengths.shape[1]
    seq_index = lax.axis_index("seq")
    mp_index = lax.axis_index("mp")
    bucket = seq_index // 4
    place = lax.rem(seq_index, 4)
    core = lax.rem(place, 2)
    chip = place // 2
    other = 1 - chip
    inputs = (query, key, value)

    def device(there_chip, there_core, there_mp):
        return {"seq": bucket * 4 + there_chip * 2 + there_core, "mp": there_mp}

    def lanes(piece, base=0):
        first, count = pieces[piece]
        return pl.ds(pl.multiple_of((base + first) * HD, HD), count * HD)

    def block_at(index):
        return pl.ds(pl.multiple_of(index * rows, rows), rows)

    def send(kind, piece, there_chip, there_core):
        return pltpu.make_async_remote_copy(
            src_ref=inputs[kind].at[:, lanes(piece, (there_core * 2 + there_chip) * wide)],
            dst_ref=kept.at[kind, block_at(place), lanes(piece)],
            send_sem=sent, recv_sem=landed.at[kind, piece],
            device_id=device(there_chip, there_core, mp_index), device_id_type=MESH,
        )

    def keep(kind, piece):
        return pltpu.make_async_copy(
            inputs[kind].at[:, lanes(piece, (core * 2 + chip) * wide)],
            kept.at[kind, block_at(place), lanes(piece)], landed.at[kind, piece],
        )

    def result(piece, there_chip, core_step, mp_step):
        there_core = core_step if there_chip is other else lax.rem(core + core_step, 2)
        there_mp = lax.rem(mp_index + mp_step, mp)
        first = (there_chip * 2 + there_core) * rows + there_mp * part
        source = results.at[pl.ds(pl.multiple_of(first, part), part), lanes(piece)]
        target = out.at[:, lanes(piece, mp_index * heads + (core * 2 + chip) * wide)]
        if there_chip is chip and core_step == 0 and mp_step == 0:
            target[...] = source[...]
            return
        pltpu.make_async_remote_copy(
            src_ref=source, dst_ref=target, send_sem=result_out, recv_sem=result_in,
            device_id=device(there_chip, there_core, there_mp), device_id_type=MESH,
        ).start()

    barrier = pltpu.get_barrier_semaphore()
    far = [device(other, b, mp_index) for b in range(2)]
    beside = [device(chip, b, lax.rem(mp_index + m, mp)) for m in range(1, mp) for b in range(2)]

    def greet(semaphore, devices):
        for there in devices:
            pl.semaphore_signal(semaphore, inc=1, device_id=there, device_id_type=MESH)

    greet(barrier, far)
    root = jnp.logical_and(chip == 0, mp_index == 0)
    leaf = jnp.logical_and(chip == 0, mp_index != 0)
    rooted = [device(0, b, 0) for b in range(2)]
    pl.when(root)(lambda: greet(barrier, beside))
    pl.semaphore_wait(barrier, len(far) + lax.select(leaf, len(rooted), 0))

    for piece in range(len(pieces)):
        for kind in (1, 0, 2):
            for there_core in range(2):
                send(kind, piece, other, there_core).start()
    fetch = pltpu.make_async_copy(lengths, table, table_in)
    fetch.start()
    for piece in range(len(pieces)):
        for kind in (1, 0, 2):
            keep(kind, piece).start()

    greet(ready, far)

    pl.when(leaf)(lambda: greet(ready, rooted))

    @pl.when(root)
    def _():
        pl.semaphore_wait(ready, len(far) + len(beside))
        greet(ready, beside)

    pl.when(leaf)(lambda: pl.semaphore_wait(ready, len(far) + len(rooted)))
    pl.when(chip == 0)(lambda: greet(ready, far))

    pl.when(chip != 0)(lambda: pl.semaphore_wait(ready, 2 * len(far)))

    for piece in range(len(pieces)):
        for kind in (1, 0, 2):
            send(kind, piece, chip, 1 - core).start()

    fetch.wait()
    ends = []
    running = jnp.int32(0)
    for i in range(slots):
        running = running + table[bucket, i]
        ends.append(running)

    def ids(offset):
        found = jnp.zeros_like(offset)
        for end in ends:
            found = found + (offset >= end).astype(jnp.int32)
        return found

    k_ids = ids(lax.broadcasted_iota(jnp.int32, (1, 4 * rows), 1))
    factor = LOG2E / HD**0.5

    def arrived(kind, piece):
        ref = kept.at[kind, :, lanes(piece)]
        pltpu.make_async_copy(ref, ref, landed.at[kind, piece]).wait()

    def heads_of(piece):
        first, count = pieces[piece]
        return [(head, slice(head * HD, (head + 1) * HD)) for head in range(first, first + count)]

    def weigh(piece, index):
        block = block_at(index)
        q_ids = ids(lax.broadcasted_iota(jnp.int32, (rows, 1), 0) + index * rows)
        for head, lane in heads_of(piece):
            score = lax.dot_general(
                kept[0, block, lane], kept[1, :, lane],
                (((1,), (1,)), ((), ())), preferred_element_type=jnp.float32,
            )
            score = jnp.where(q_ids == k_ids, score, NEG)
            top = jnp.max(score, axis=1, keepdims=True)
            weight = jnp.exp2((score - top) * factor)
            totals[head, block, :] = jnp.broadcast_to(jnp.sum(weight, axis=1, keepdims=True), (rows, HD))
            weights[head, block, :] = weight.astype(jnp.bfloat16)

    def attend(piece, index, count=1):
        block = pl.ds(pl.multiple_of(index * count * rows, count * rows), count * rows)
        for head, lane in heads_of(piece):
            summed = jnp.dot(weights[head, block, :], kept[2, :, lane], preferred_element_type=jnp.float32)
            results[block, lane] = (summed / totals[head, block, :]).astype(jnp.bfloat16)

    def direct(piece):
        for core_step in range(2):
            result(piece, other, core_step, 0)

    def diagonal(piece, cores=(0, 1)):
        for mp_step in range(1, mp):
            for core_step in cores:
                result(piece, other, core_step, mp_step)

    def own(piece):
        for core_step in reversed(range(2)):
            for mp_step in reversed(range(mp)):
                result(piece, chip, core_step, mp_step)

    def each(work, piece, there_chip):
        @pl.loop(0, 2)
        def _(step):
            work(piece, there_chip * 2 + step)

    last = len(pieces) - 1
    for piece in range(len(pieces)):
        arrived(1, piece)
        arrived(0, piece)
        each(weigh, piece, other)
        if piece < last:
            each(weigh, piece, chip)
        if piece:
            both = jnp.logical_and(mp_index == 1, chip == 1)
            pl.when(mp_index == 1)(lambda: diagonal(piece - 1, (0,)))
            pl.when(both)(lambda: diagonal(piece - 1, (1,)))
        if piece == last:
            each(weigh, piece, chip)
        arrived(2, piece)
        if piece:
            pl.when(mp_index != 1)(lambda: diagonal(piece - 1, (0,)))
            pl.when(jnp.logical_not(both))(lambda: diagonal(piece - 1, (1,)))
        if piece == last:
            attend(piece, other, 2)
        else:
            each(attend, piece, other)
        direct(piece)
        if piece == last:
            diagonal(piece)
        each(attend, piece, chip)
        own(piece)

    whole = kept.at[:, pl.ds(0, 3 * rows)]
    pltpu.make_async_copy(whole, whole, sent).wait()
    moved = out.at[:, pl.ds(0, out.shape[1] - wide * HD)]
    pltpu.make_async_copy(moved, moved, result_out).wait()
    pltpu.make_async_copy(moved, moved, result_in).wait()


def duo_call(query, key, value, clip_lengths):
    rows, width = query.shape
    heads = width // HD
    mp = lax.axis_size("mp")
    wide = heads // 4
    early = (wide + 1) // 2
    pieces = [(0, early)] + [(head, 1) for head in range(early, wide)]
    dma = pltpu.SemaphoreType.DMA
    whole = pl.BlockSpec(memory_space=pl.ANY)
    return pl.pallas_call(
        functools.partial(duo, heads, pieces),
        out_shape=pltpu.VMEM((rows // mp, width * mp), jnp.bfloat16),
        in_specs=[whole] * 4,
        out_specs=pl.BlockSpec(memory_space=pltpu.VMEM),
        scratch_shapes=[
            pltpu.VMEM((3, 4 * rows, wide * HD), jnp.bfloat16),
            pltpu.VMEM((wide, 4 * rows, 4 * rows), jnp.bfloat16),
            pltpu.VMEM((wide, 4 * rows, HD), jnp.float32),
            pltpu.VMEM((4 * rows, wide * HD), jnp.bfloat16),
            pltpu.SMEM(clip_lengths.shape, jnp.int32),
            dma((3, len(pieces))), dma(()), dma(()), dma(()), dma(()), pltpu.SemaphoreType.REGULAR,
        ],
        compiler_params=pltpu.CompilerParams(collective_id=0, has_side_effects=True),
        name="packed_attention",
    )(clip_lengths, query, key, value)


def shards(query, key, value, clip_lengths):
    rows, width = query.shape
    heads = width // HD
    group = lax.axis_size("seq") // clip_lengths.shape[0]
    mp = lax.axis_size("mp")
    if group == 4 and heads % 4 == 0 and rows % (16 * mp) == 0 and mp > 1:
        return duo_call(query, key, value, clip_lengths)
    pair = 2 if group % 2 == 0 and heads % 2 == 0 else 1
    per_core = heads // pair
    others = group // pair
    lead = min(2, (per_core - 1) // others) if others > 1 else 0
    held = per_core - lead * (others - 1)
    dma = pltpu.SemaphoreType.DMA
    whole = pl.BlockSpec(memory_space=pl.ANY)
    return pl.pallas_call(
        functools.partial(kernel, group, pair, mp, heads, lead),
        out_shape=pltpu.VMEM((rows // mp, width * mp), jnp.bfloat16),
        in_specs=[pl.BlockSpec(memory_space=pltpu.SMEM), whole, whole, whole],
        out_specs=pl.BlockSpec(memory_space=pltpu.VMEM),
        scratch_shapes=[
            pltpu.VMEM((held, group * rows, HD), jnp.bfloat16),
            pltpu.VMEM((held, group * rows, HD), jnp.bfloat16),
            pltpu.VMEM((held, group * rows, HD), jnp.bfloat16),
            pltpu.VMEM((per_core, pair * rows, HD), jnp.bfloat16),
            pltpu.VMEM((3, group, rows, HD), jnp.bfloat16),
            pltpu.VMEM((pair * rows, group * rows), jnp.bfloat16),
            pltpu.VMEM((pair * rows, HD), jnp.float32),
            dma((held, group)), dma((held, group)), dma((held, group)), dma((per_core, pair * mp)),
            dma((held, group)), dma((held, group)), dma((held, group)), dma((per_core, pair * mp)),
            dma((3, group)), pltpu.SemaphoreType.REGULAR,
        ],
        compiler_params=pltpu.CompilerParams(collective_id=0, has_side_effects=True),
        name="packed_attention",
    )(clip_lengths, query, key, value)


def solution(mesh):
    in_specs = (P("seq", "mp"), P("seq", "mp"), P("seq", "mp"), P())
    out_specs = P(("seq", "mp"), None)
    return jax.shard_map(shards, mesh=mesh, in_specs=in_specs, out_specs=out_specs, check_vma=False)
```
